32 devices in a mesh: dp: 1 (over z), tp: 4 (over y), sp: 8 (over x, core).
Axes of the slice: x: 4, y: 4, z: 1, core: 2. Of those that a mesh axis runs over, the one named last changes fastest.
The devices are a block of a 4x4x8 slice.
Arguments:
- x_in: bfloat16 [131072, 512], P(('dp', 'sp'))
- grad_y: bfloat16 [131072, 512], P(('dp', 'sp'))
- w_qkv: bfloat16 [512, 3, 512], P(None, None, 'tp')
- w_out: bfloat16 [512, 512], P('tp')
- ln_gamma: float32 [512], replicated
- ln_beta: float32 [512], replicated
- temperature: float32 [8], replicated
Outputs:
- output 1: bfloat16 [131072, 512], P(('dp', 'sp'))
- output 2: bfloat16 [131072, 512], P(('dp', 'sp'))
- output 3: float32 [512, 3, 512], P(('dp', 'sp'), None, 'tp')
- output 4: float32 [512, 512], P(('dp', 'tp', 'sp'))
- output 5: float32 [512], P('dp')
- output 6: float32 [512], P('dp')
- output 7: float32 [8], P('dp')
All inputs are finite; a program needn't handle non-finite values.
Results may differ from the reference program's by a relative error of at most 0.001.
Values are sent between devices in bfloat16 or wider.
A program may use at most 768 MiB of HBM per device.

```python
import jax
import jax.numpy as jnp
from jax import lax

MODEL_DIM = 512
NUM_HEADS = 8
NUM_TOKENS = 131072
NUM_REGIONS = 8
HEAD_DIM = MODEL_DIM // NUM_HEADS
LN_EPS = 1e-6


def setup_inputs(seed: int = 0, part: int = 0) -> dict:
    part_key = jax.random.fold_in(jax.random.key(seed), part)
    key_noise, key_offset, key_grad, key_goffset = jax.random.split(part_key, 4)
    key_wqkv, key_wout, key_gamma, key_beta, key_temp = jax.random.split(jax.random.key(seed + 1), 5)
    rows_per_region = NUM_TOKENS // NUM_REGIONS
    w_scale = MODEL_DIM ** -0.5
    offsets = jax.random.normal(key_offset, (NUM_REGIONS, MODEL_DIM), jnp.float32)
    x_vals = jax.random.normal(key_noise, (NUM_TOKENS, MODEL_DIM), jnp.float32) + jnp.repeat(offsets, rows_per_region, axis=0)
    grad_offsets = 0.5 * jax.random.normal(key_goffset, (NUM_REGIONS, MODEL_DIM), jnp.float32)
    grad_vals = jax.random.normal(key_grad, (NUM_TOKENS, MODEL_DIM), jnp.float32) + jnp.repeat(grad_offsets, rows_per_region, axis=0)
    w_qkv = jax.random.normal(key_wqkv, (MODEL_DIM, 3, MODEL_DIM), jnp.float32) * w_scale
    w_out = jax.random.normal(key_wout, (MODEL_DIM, MODEL_DIM), jnp.float32) * w_scale
    ln_gamma = 1.0 + 0.3 * jax.random.normal(key_gamma, (MODEL_DIM,), jnp.float32)
    ln_beta = 0.3 * jax.random.normal(key_beta, (MODEL_DIM,), jnp.float32)
    temperature = jax.random.uniform(key_temp, (NUM_HEADS,), jnp.float32, 2.0, 4.0)
    return {"x_in": x_vals.astype(jnp.bfloat16), "grad_y": grad_vals.astype(jnp.bfloat16), "w_qkv": w_qkv.astype(jnp.bfloat16), "w_out": w_out.astype(jnp.bfloat16), "ln_gamma": ln_gamma, "ln_beta": ln_beta, "temperature": temperature}


def head_pass(operands):
    q_head, k_head, v_head, dout_head, temp_one = operands
    gram_mat = jnp.dot(q_head.T, k_head, preferred_element_type=jnp.float32)
    q_sq = jnp.sum(jnp.square(q_head.astype(jnp.float32)), axis=0)
    k_sq = jnp.sum(jnp.square(k_head.astype(jnp.float32)), axis=0)
    norm_prod = jnp.sqrt(q_sq)[:, None] * jnp.sqrt(k_sq)[None, :]
    gram_n = gram_mat / norm_prod
    attn_prob = jax.nn.softmax(temp_one * gram_n, axis=-1)
    attn_bf = attn_prob.astype(jnp.bfloat16)
    out_head = jnp.dot(v_head, attn_bf.T, preferred_element_type=jnp.float32).astype(jnp.bfloat16)
    d_attn = jnp.dot(dout_head.T, v_head, preferred_element_type=jnp.float32)
    dv_head = jnp.dot(dout_head, attn_bf, preferred_element_type=jnp.float32).astype(jnp.bfloat16)
    d_logit = attn_prob * (d_attn - jnp.sum(attn_prob * d_attn, axis=-1, keepdims=True))
    temp_grad = jnp.sum(d_logit * gram_n)
    grad_sn = temp_one * d_logit
    d_gram = (grad_sn / norm_prod).astype(jnp.bfloat16)
    prod_sn = grad_sn * gram_n
    q_coef = -jnp.sum(prod_sn, axis=1) / q_sq
    k_coef = -jnp.sum(prod_sn, axis=0) / k_sq
    dq_head = (jnp.dot(k_head, d_gram.T, preferred_element_type=jnp.float32) + q_head.astype(jnp.float32) * q_coef[None, :]).astype(jnp.bfloat16)
    dk_head = (jnp.dot(q_head, d_gram, preferred_element_type=jnp.float32) + k_head.astype(jnp.float32) * k_coef[None, :]).astype(jnp.bfloat16)
    return out_head, dq_head, dk_head, dv_head, temp_grad


def reference(x_in, grad_y, w_qkv, w_out, ln_gamma, ln_beta, temperature):
    x_float = x_in.astype(jnp.float32)
    centered = x_float - jnp.mean(x_float, axis=1, keepdims=True)
    inv_std = lax.rsqrt(jnp.mean(centered * centered, axis=1, keepdims=True) + LN_EPS)
    x_hat = centered * inv_std
    u_act = (x_hat * ln_gamma + ln_beta).astype(jnp.bfloat16)
    w_flat = w_qkv.reshape(MODEL_DIM, 3 * MODEL_DIM)
    qkv_act = jnp.dot(u_act, w_flat, preferred_element_type=jnp.float32).astype(jnp.bfloat16)
    qkv_heads = qkv_act.reshape(NUM_TOKENS, 3, NUM_HEADS, HEAD_DIM).transpose(1, 2, 0, 3)
    dout_act = jnp.dot(grad_y, w_out.T, preferred_element_type=jnp.float32).astype(jnp.bfloat16)
    dout_heads = dout_act.reshape(NUM_TOKENS, NUM_HEADS, HEAD_DIM).transpose(1, 0, 2)
    out_heads, dq_heads, dk_heads, dv_heads, grad_temp = lax.map(head_pass, (qkv_heads[0], qkv_heads[1], qkv_heads[2], dout_heads, temperature))
    out_act = out_heads.transpose(1, 0, 2).reshape(NUM_TOKENS, MODEL_DIM)
    y_out = (x_float + jnp.dot(out_act, w_out, preferred_element_type=jnp.float32)).astype(jnp.bfloat16)
    grad_wout = jnp.dot(out_act.T, grad_y, preferred_element_type=jnp.float32)
    dqkv_act = jnp.stack([dq_heads, dk_heads, dv_heads], axis=0).transpose(2, 0, 1, 3).reshape(NUM_TOKENS, 3 * MODEL_DIM)
    grad_wqkv = jnp.dot(u_act.T, dqkv_act, preferred_element_type=jnp.float32).reshape(MODEL_DIM, 3, MODEL_DIM)
    grad_u = jnp.dot(dqkv_act, w_flat.T, preferred_element_type=jnp.float32)
    grad_gamma = jnp.sum(grad_u * x_hat, axis=0)
    grad_beta = jnp.sum(grad_u, axis=0)
    grad_xhat = grad_u * ln_gamma
    grad_ln = inv_std * (grad_xhat - jnp.mean(grad_xhat, axis=1, keepdims=True) - x_hat * jnp.mean(grad_xhat * x_hat, axis=1, keepdims=True))
    grad_x = (grad_y.astype(jnp.float32) + grad_ln).astype(jnp.bfloat16)
    return y_out, grad_x, grad_wqkv, grad_wout, grad_gamma, grad_beta, grad_temp
```

```python
import functools

import jax
import jax.numpy as jnp
from jax import lax
from jax.experimental import pallas as pl
from jax.experimental.pallas import tpu as pltpu
from jax.sharding import PartitionSpec as P

LN_EPS = 1e-6
F32 = jnp.float32
BF16 = jnp.bfloat16
MESH = pl.DeviceIdType.MESH
STATS_ROWS = 512
MAIN_ROWS = 512


def dot(lhs, rhs):
    return jnp.dot(lhs, rhs, preferred_element_type=F32)


def dot_rows(lhs, rhs):
    return lax.dot_general(lhs, rhs, (((0,), (0,)), ((), ())), preferred_element_type=F32)


def layer_norm(x, gamma, beta):
    centered = x - jnp.mean(x, axis=-1, keepdims=True)
    inv_std = lax.rsqrt(jnp.mean(centered * centered, axis=-1, keepdims=True) + LN_EPS)
    x_hat = centered * inv_std
    return x_hat, inv_std, (x_hat * gamma + beta).astype(BF16)


def stats_kernel(cols, x_ref, g_ref, w_ref, gamma_ref, beta_ref, qk_ref, dv_ref):
    @pl.when(pl.program_id(0) == 0)
    def _():
        qk_ref[...] = jnp.zeros_like(qk_ref)
        dv_ref[...] = jnp.zeros_like(dv_ref)

    _, _, u = layer_norm(x_ref[...].astype(F32), gamma_ref[...], beta_ref[...])
    qkv = dot(u, w_ref[:, : 3 * cols]).astype(BF16)
    dout = dot(g_ref[...], w_ref[:, 3 * cols :]).astype(BF16)
    qk = qkv[:, : 2 * cols]
    qk_ref[...] += dot_rows(qk, qk)
    dv_ref[...] += dot_rows(dout, qkv[:, 2 * cols :])


def run_stats(x, g, w, gamma, beta):
    tokens, width = x.shape
    cols = w.shape[1] // 4
    rows = STATS_ROWS
    tile = pl.BlockSpec((rows, width), lambda i: (i, 0))
    whole = lambda shape: pl.BlockSpec(shape, lambda i: (0, 0))
    return pl.pallas_call(
        functools.partial(stats_kernel, cols),
        grid=(tokens // rows,),
        out_shape=(
            jax.ShapeDtypeStruct((2 * cols, 2 * cols), F32),
            jax.ShapeDtypeStruct((cols, cols), F32),
        ),
        in_specs=[tile, tile, whole(w.shape), whole((1, width)), whole((1, width))],
        out_specs=(whole((2 * cols, 2 * cols)), whole((cols, cols))),
        compiler_params=pltpu.CompilerParams(dimension_semantics=("arbitrary",), vmem_limit_bytes=40 << 20),
        cost_estimate=pl.CostEstimate(
            flops=2 * tokens * width * 6 * cols, bytes_accessed=4 * tokens * width, transcendentals=0
        ),
        name="stats",
    )(x, g, w, gamma, beta)


def state_kernel(
    n_sp, n_tp, qk_ref, dv_ref, temp_ref, mats_ref, rows_ref, gt_ref,
    gath, mats, rows, sp_send, sp_recv, tp_send, tp_recv,
):
    me_s, me_t = lax.axis_index("sp"), lax.axis_index("tp")
    cols = dv_ref.shape[0]
    hd = cols // 2
    barrier = pltpu.get_barrier_semaphore()
    for d in range(1, n_sp):
        pl.semaphore_signal(barrier, inc=1, device_id={"sp": lax.rem(me_s + d, n_sp)}, device_id_type=MESH)
    for d in range(1, n_tp):
        pl.semaphore_signal(barrier, inc=1, device_id={"tp": lax.rem(me_t + d, n_tp)}, device_id_type=MESH)

    lane = lax.broadcasted_iota(jnp.int32, (hd, cols), 1)
    first = lane < hd
    eye = lax.broadcasted_iota(jnp.int32, (cols, cols), 0) == lax.broadcasted_iota(jnp.int32, (cols, cols), 1)

    def fold(block):
        return jnp.where(first, block[:hd], block[hd:])

    def diag_row(block):
        return jnp.sum(jnp.where(eye, block, 0.0), axis=0, keepdims=True)

    gath[0, :hd] = fold(qk_ref[:cols, cols:])
    gath[0, hd : 2 * hd] = fold(dv_ref[...])
    gath[0, 2 * hd : 2 * hd + 8] = jnp.concatenate(
        [diag_row(qk_ref[:cols, :cols]), diag_row(qk_ref[cols:, cols:]), jnp.zeros((6, cols), F32)], axis=0
    )
    pl.semaphore_wait(barrier, n_sp + n_tp - 2)

    copies = []
    for d in range(1, n_sp):
        copy = pltpu.make_async_remote_copy(
            src_ref=gath.at[0], dst_ref=gath.at[d], send_sem=sp_send.at[d], recv_sem=sp_recv.at[d],
            device_id={"sp": lax.rem(me_s + d, n_sp)}, device_id_type=MESH,
        )
        copy.start()
        copies.append(copy)
    for copy in copies:
        copy.wait()
    total = gath[me_s]
    for s in range(1, n_sp):
        total = total + gath[lax.rem(me_s - s + n_sp, n_sp)]

    gram, d_attn = total[:hd], total[hd : 2 * hd]
    q_row, k_row = total[2 * hd : 2 * hd + 1], total[2 * hd + 1 : 2 * hd + 2]
    q_all = jnp.sum(jnp.where(eye, jnp.broadcast_to(q_row, (cols, cols)), 0.0), axis=1, keepdims=True)
    q_col = jnp.where(first, jnp.broadcast_to(q_all[:hd], (hd, cols)), jnp.broadcast_to(q_all[hd:], (hd, cols)))
    heads = [temp_ref[2 * me_t], temp_ref[2 * me_t + 1]]
    temp = jnp.where(first, heads[0], heads[1])

    def per_head(value, reduce, other):
        lo = reduce(jnp.where(first, value, other), axis=1, keepdims=True)
        hi = reduce(jnp.where(first, other, value), axis=1, keepdims=True)
        return jnp.where(first, jnp.broadcast_to(lo, (hd, cols)), jnp.broadcast_to(hi, (hd, cols)))

    norm = jnp.sqrt(q_col) * jnp.sqrt(k_row)
    gram_n = gram / norm
    logit = temp * gram_n
    expo = jnp.exp(logit - per_head(logit, jnp.max, -jnp.inf))
    attn = expo / per_head(expo, jnp.sum, 0.0)
    d_logit = attn * (d_attn - per_head(attn * d_attn, jnp.sum, 0.0))
    temp_part = jnp.sum(per_head(d_logit * gram_n, jnp.sum, 0.0), axis=0, keepdims=True)
    grad_sn = temp * d_logit
    prod = grad_sn * gram_n
    same = lax.broadcasted_iota(jnp.int32, (hd, cols), 0) == lax.rem(lane, hd)
    q_coef = jnp.sum(jnp.where(same, -per_head(prod, jnp.sum, 0.0) / q_col, 0.0), axis=0, keepdims=True)
    k_coef = -jnp.sum(prod, axis=0, keepdims=True) / k_row

    mats[0, :hd] = attn.astype(BF16)
    mats[0, hd:] = (grad_sn / norm).astype(BF16)
    rows[0] = jnp.concatenate([q_coef, k_coef, temp_part, jnp.zeros((5, cols), F32)], axis=0)
    copies = []
    for d in range(1, n_tp):
        for k, ref in enumerate((mats, rows)):
            copy = pltpu.make_async_remote_copy(
                src_ref=ref.at[0], dst_ref=ref.at[d], send_sem=tp_send.at[k, d], recv_sem=tp_recv.at[k, d],
                device_id={"tp": lax.rem(me_t + d, n_tp)}, device_id_type=MESH,
            )
            copy.start()
            copies.append(copy)
    for copy in copies:
        copy.wait()
    for t in range(n_tp):
        slot = lax.rem(me_t - t + n_tp, n_tp)
        mats_ref[t] = mats[slot]
        part = rows[slot]
        rows_ref[t] = part
        gt_ref[2 * t] = part[2, 0]
        gt_ref[2 * t + 1] = part[2, hd]


def run_state(n_sp, n_tp, qk, dv, temp):
    cols = dv.shape[0]
    n_rows = cols + 8
    vmem = pl.BlockSpec(memory_space=pltpu.VMEM)
    smem = pl.BlockSpec(memory_space=pltpu.SMEM)
    dma = pltpu.SemaphoreType.DMA
    return pl.pallas_call(
        functools.partial(state_kernel, n_sp, n_tp),
        out_shape=(
            jax.ShapeDtypeStruct((n_tp, cols, cols), BF16),
            jax.ShapeDtypeStruct((n_tp, 8, cols), F32),
            jax.ShapeDtypeStruct(temp.shape, F32),
        ),
        in_specs=[vmem, vmem, smem],
        out_specs=(vmem, vmem, smem),
        scratch_shapes=[
            pltpu.VMEM((n_sp, n_rows, cols), F32),
            pltpu.VMEM((n_tp, cols, cols), BF16),
            pltpu.VMEM((n_tp, 8, cols), F32),
            dma((n_sp,)), dma((n_sp,)), dma((2, n_tp)), dma((2, n_tp)),
        ],
        compiler_params=pltpu.CompilerParams(collective_id=0, has_side_effects=True),
        name="state",
    )(qk, dv, temp)


def main_kernel(
    n_tp, t_ref, x_ref, g_ref, w0_ref, w1_ref, w2_ref, w3_ref, mats_ref, rows_ref, gamma_ref, beta_ref,
    y_ref, dx_ref, dw_ref, dwo_ref, dgb_ref,
    w_s, wt_s, wo_s, wot_s, at_s, a_s, gt_s, g_s, co_s, u_s, r_s, o_s, own_s, dwt_s,
):
    width = x_ref.shape[1]
    cols = width // n_tp
    hd = cols // 2
    me_t = t_ref[0]
    step = pl.program_id(0)

    @pl.when(step == 0)
    def _():
        for i, ref in enumerate((w0_ref, w1_ref, w2_ref, w3_ref)):
            at = pl.multiple_of(lax.rem(me_t + i, n_tp) * cols, cols)
            for e in range(3):
                block = ref[:, e * cols : (e + 1) * cols]
                w_s[:, pl.ds(e * width + at, cols)] = block
                wt_s[pl.ds(e * width + at, cols), :] = block.T
            block = ref[:, 3 * cols :]
            wot_s[:, pl.ds(at, cols)] = block
            wo_s[pl.ds(at, cols), :] = block.T
        for ref in (at_s, a_s, gt_s, g_s):
            ref[...] = jnp.zeros_like(ref)
        first = lax.broadcasted_iota(jnp.int32, (hd, cols), 1) < hd
        for t in range(n_tp):
            p, off = t // 2, (t % 2) * cols
            for k, (plain, trans) in enumerate(((a_s, at_s), (g_s, gt_s))):
                block = mats_ref[t, k * hd : (k + 1) * hd].astype(F32)
                full = jnp.concatenate([jnp.where(first, block, 0.0), jnp.where(first, 0.0, block)], axis=0)
                plain[p, off : off + cols, off : off + cols] = full.astype(BF16)
                trans[p, off : off + cols, off : off + cols] = full.T.astype(BF16)
            co_s[0:1, t * cols : (t + 1) * cols] = rows_ref[t, 0:1]
            co_s[1:2, t * cols : (t + 1) * cols] = rows_ref[t, 1:2]
        dwt_s[...] = jnp.zeros_like(dwt_s)
        dwo_ref[...] = jnp.zeros_like(dwo_ref)
        dgb_ref[...] = jnp.zeros_like(dgb_ref)

    gamma = gamma_ref[...]
    x = x_ref[...].astype(F32)
    x_hat, inv_std, u = layer_norm(x, gamma, beta_ref[...])
    u_s[...] = u
    for p in range(2):
        lo, hi = p * 2 * cols, (p + 1) * 2 * cols
        q = dot(u_s[...], w_s[:, lo:hi]).astype(BF16)
        k = dot(u_s[...], w_s[:, width + lo : width + hi]).astype(BF16)
        v = dot(u_s[...], w_s[:, 2 * width + lo : 2 * width + hi]).astype(BF16)
        dout = dot(g_ref[...], wot_s[:, lo:hi]).astype(BF16)
        o_s[:, lo:hi] = dot(v, at_s[p]).astype(BF16)
        r_s[:, 2 * width + lo : 2 * width + hi] = dot(dout, a_s[p]).astype(BF16)
        r_s[:, lo:hi] = (dot(k, gt_s[p]) + q.astype(F32) * co_s[0:1, lo:hi]).astype(BF16)
        r_s[:, width + lo : width + hi] = (dot(q, g_s[p]) + k.astype(F32) * co_s[1:2, lo:hi]).astype(BF16)
    y_ref[...] = (x + dot(o_s[...], wo_s[...])).astype(BF16)
    du = dot(r_s[...], wt_s[...])
    dgb_ref[0:1] += jnp.sum(du * x_hat, axis=0, keepdims=True)
    dgb_ref[1:2] += jnp.sum(du, axis=0, keepdims=True)
    gx = du * gamma
    mean1 = jnp.mean(gx, axis=-1, keepdims=True)
    mean2 = jnp.mean(gx * x_hat, axis=-1, keepdims=True)
    dx_ref[...] = (g_ref[...].astype(F32) + inv_std * (gx - mean1 - x_hat * mean2)).astype(BF16)

    mine = pl.multiple_of(me_t * cols, cols)
    for e in range(3):
        own_s[:, e * cols : (e + 1) * cols] = r_s[:, pl.ds(e * width + mine, cols)]
    dwt_s[...] += dot_rows(own_s[...], u_s[...])
    dwo_ref[...] += dot_rows(o_s[:, pl.ds(mine, cols)], g_ref[...])

    @pl.when(step == pl.num_programs(0) - 1)
    def _():
        for e in range(3):
            dw_ref[:, e * cols : (e + 1) * cols] = dwt_s[e * cols : (e + 1) * cols, :].T


def run_main(n_tp, me_t, x, g, ws, mats, rows, gamma, beta):
    tokens, width = x.shape
    cols = width // n_tp
    r = MAIN_ROWS
    tile = pl.BlockSpec((r, width), lambda i, t: (i, 0))

    def whole(shape):
        return pl.BlockSpec(shape, lambda i, t: (0,) * len(shape))

    vmem = pltpu.VMEM
    pair = (2, 2 * cols, 2 * cols)
    return pl.pallas_call(
        functools.partial(main_kernel, n_tp),
        grid_spec=pltpu.PrefetchScalarGridSpec(
            num_scalar_prefetch=1,
            grid=(tokens // r,),
            in_specs=[tile, tile] + [whole(w.shape) for w in ws]
            + [whole(mats.shape), whole(rows.shape), whole((1, width)), whole((1, width))],
            out_specs=(tile, tile, whole((width, 3 * cols)), whole((cols, width)), whole((8, width))),
            scratch_shapes=[
                vmem((width, 3 * width), BF16), vmem((3 * width, width), BF16),
                vmem((width, width), BF16), vmem((width, width), BF16),
                vmem(pair, BF16), vmem(pair, BF16), vmem(pair, BF16), vmem(pair, BF16),
                vmem((8, width), F32),
                vmem((r, width), BF16), vmem((r, 3 * width), BF16), vmem((r, width), BF16), vmem((r, 3 * cols), BF16),
                vmem((3 * cols, width), F32),
            ],
        ),
        out_shape=(
            jax.ShapeDtypeStruct(x.shape, BF16),
            jax.ShapeDtypeStruct(x.shape, BF16),
            jax.ShapeDtypeStruct((width, 3 * cols), F32),
            jax.ShapeDtypeStruct((cols, width), F32),
            jax.ShapeDtypeStruct((8, width), F32),
        ),
        compiler_params=pltpu.CompilerParams(dimension_semantics=("arbitrary",), vmem_limit_bytes=60 << 20),
        cost_estimate=pl.CostEstimate(
            flops=2 * tokens * width * width * 11, bytes_accessed=8 * tokens * width, transcendentals=0
        ),
        name="main",
    )(me_t, x, g, *ws, mats, rows, gamma, beta)


def reduce_kernel(
    n_chip, dw_ref, dwo_ref, dgb_ref, dw_out, dwo_out, dg_out, db_out,
    got_w, got_o, got_g, sum_w, sum_o, sum_g, in_w, in_o, in_g, a_send, a_recv, b_send, b_recv,
):
    me = lax.axis_index("sp")
    core, chip = lax.rem(me, 2), me // 2
    partner = me + 1 - 2 * core
    barrier = pltpu.get_barrier_semaphore()
    pl.semaphore_signal(barrier, inc=1, device_id={"sp": partner}, device_id_type=MESH)
    peers = [2 * lax.rem(chip + d, n_chip) + core for d in range(n_chip)]
    for d in range(1, n_chip):
        pl.semaphore_signal(barrier, inc=1, device_id={"sp": peers[d]}, device_id_type=MESH)
    pl.semaphore_wait(barrier, n_chip)

    copies = []
    for k, (src, dst) in enumerate(
        ((dw_ref.at[:, 1 - core], got_w), (dwo_ref.at[:, 1 - core], got_o), (dgb_ref, got_g))
    ):
        copy = pltpu.make_async_remote_copy(
            src_ref=src, dst_ref=dst, send_sem=a_send.at[k], recv_sem=a_recv.at[k],
            device_id={"sp": partner}, device_id_type=MESH,
        )
        copy.start()
        copies.append(copy)
    for copy in copies:
        copy.wait()
    sum_w[...] = dw_ref[:, core] + got_w[...]
    sum_o[...] = dwo_ref[:, core] + got_o[...]
    sum_g[...] = dgb_ref[...] + got_g[...]
    in_g[0] = sum_g[...]
    copies = []
    for d in range(1, n_chip):
        to = lax.rem(chip + d, n_chip)
        for k, (src, dst) in enumerate(((sum_w.at[to], in_w.at[d]), (sum_o.at[to], in_o.at[d]), (sum_g, in_g.at[d]))):
            copy = pltpu.make_async_remote_copy(
                src_ref=src, dst_ref=dst, send_sem=b_send.at[k, d], recv_sem=b_recv.at[k, d],
                device_id={"sp": peers[d]}, device_id_type=MESH,
            )
            copy.start()
            copies.append(copy)
    for copy in copies:
        copy.wait()
    w_tot, o_tot, g_tot = sum_w[chip], sum_o[chip], in_g[chip]
    for d in range(1, n_chip):
        w_tot = w_tot + in_w[d]
        o_tot = o_tot + in_o[d]
        g_tot = g_tot + in_g[lax.rem(chip - d + n_chip, n_chip)]
    cols = w_tot.shape[1] // 3
    for e in range(3):
        dw_out[:, e, :] = w_tot[:, e * cols : (e + 1) * cols]
    dwo_out[...] = o_tot
    dg_out[...] = g_tot[0:1]
    db_out[...] = g_tot[1:2]


def run_reduce(n_sp, dw, dwo, dgb):
    width, cols3 = dw.shape
    cols = dwo.shape[0]
    n_chip = n_sp // 2
    dw = dw.reshape(n_chip, 2, width // n_sp, cols3)
    dwo = dwo.reshape(n_chip, 2, cols // n_sp, width)
    w_shape, o_shape, g_shape = (n_chip,) + dw.shape[2:], (n_chip,) + dwo.shape[2:], dgb.shape
    vmem = pl.BlockSpec(memory_space=pltpu.VMEM)
    dma = pltpu.SemaphoreType.DMA
    return pl.pallas_call(
        functools.partial(reduce_kernel, n_chip),
        out_shape=(
            jax.ShapeDtypeStruct((width // n_sp, 3, cols3 // 3), F32),
            jax.ShapeDtypeStruct((cols // n_sp, width), F32),
            jax.ShapeDtypeStruct((1, width), F32),
            jax.ShapeDtypeStruct((1, width), F32),
        ),
        in_specs=[vmem] * 3,
        out_specs=(vmem,) * 4,
        scratch_shapes=[
            pltpu.VMEM(w_shape, F32), pltpu.VMEM(o_shape, F32), pltpu.VMEM(g_shape, F32),
            pltpu.VMEM(w_shape, F32), pltpu.VMEM(o_shape, F32), pltpu.VMEM(g_shape, F32),
            pltpu.VMEM(w_shape, F32), pltpu.VMEM(o_shape, F32), pltpu.VMEM((n_chip,) + g_shape, F32),
            dma((3,)), dma((3,)), dma((3, n_chip)), dma((3, n_chip)),
        ],
        compiler_params=pltpu.CompilerParams(collective_id=1, has_side_effects=True),
        name="reduce",
    )(dw, dwo, dgb)


def solution(mesh):
    n_tp, n_sp = mesh.shape["tp"], mesh.shape["sp"]
    row_spec = P(("dp", "sp"), None)

    def local_step(x, g, w_qkv, w_out, ln_gamma, ln_beta, temperature):
        width = x.shape[1]
        gamma, beta = ln_gamma.reshape(1, width), ln_beta.reshape(1, width)
        me_t = lax.axis_index("tp").astype(jnp.int32).reshape(1)
        w_own = jnp.concatenate([w_qkv.reshape(width, -1), w_out.T], axis=1)
        ws = [w_own]
        for d in range(1, n_tp):
            ws.append(lax.ppermute(w_own, "tp", [((i + d) % n_tp, i) for i in range(n_tp)]))
        qk, dv = run_stats(x, g, w_own, gamma, beta)
        mats, rows, grad_temp = run_state(n_sp, n_tp, qk, dv, temperature)
        y, dx, dw, dwo, dgb = run_main(n_tp, me_t, x, g, ws, mats, rows, gamma, beta)
        dw, dwo, dgamma, dbeta = run_reduce(n_sp, dw, dwo, dgb)
        return y, dx, dw, dwo, dgamma.reshape(-1), dbeta.reshape(-1), grad_temp

    in_specs = (row_spec, row_spec, P(None, None, "tp"), P("tp", None), P(None), P(None), P(None))
    out_specs = (row_spec, row_spec, P(("dp", "sp"), None, "tp"), P(("dp", "tp", "sp"), None), P("dp"), P("dp"), P("dp"))
    return jax.shard_map(local_step, mesh=mesh, in_specs=in_specs, out_specs=out_specs, check_vma=False)
```

```python
import functools

import jax
import jax.numpy as jnp
from jax import lax
from jax.experimental import pallas as pl
from jax.experimental.pallas import tpu as pltpu
from jax.sharding import PartitionSpec as P

LN_EPS = 1e-6
F32 = jnp.float32
BF16 = jnp.bfloat16
MESH = pl.DeviceIdType.MESH
STATS_ROWS = 2048
STATS_SUB = 512
MAIN_ROWS = 2048
MAIN_SUB = 512


def dot(lhs, rhs):
    return jnp.dot(lhs, rhs, preferred_element_type=F32)


def dot_rows(lhs, rhs):
    return lax.dot_general(lhs, rhs, (((0,), (0,)), ((), ())), preferred_element_type=F32)


def layer_norm(x, gamma, beta):
    centered = x - jnp.mean(x, axis=-1, keepdims=True)
    inv_std = lax.rsqrt(jnp.mean(centered * centered, axis=-1, keepdims=True) + LN_EPS)
    x_hat = centered * inv_std
    return x_hat, inv_std, (x_hat * gamma + beta).astype(BF16)


def state_kernel(
    n_sp, n_tp, x_ref, g_ref, w_ref, wo_ref, gamma_ref, beta_ref, temp_ref, w_any, wo_any,
    w_all, wo_all, mats_ref, rows_ref, gt_ref,
    w_s, u_s, qk_s, dv_s, pair, gath, mats, rows,
    w_send, w_recv, w_local, pair_send, pair_recv, sp_send, sp_recv, tp_send, tp_recv,
):
    step = pl.program_id(0)
    me_s, me_t = lax.axis_index("sp"), lax.axis_index("tp")
    n_chip = n_sp // 2
    core, chip = lax.rem(me_s, 2), me_s // 2
    cols, width = wo_ref.shape
    hd = cols // 2
    partner = {"sp": me_s + 1 - 2 * core}
    chips = [{"sp": 2 * lax.rem(chip + d, n_chip) + core} for d in range(n_chip)]
    tps = [{"tp": lax.rem(me_t + d, n_tp)} for d in range(n_tp)]

    def weight_copies():
        for d in range(1, n_tp):
            for k, (src, dst) in enumerate(((w_any, w_all), (wo_any, wo_all))):
                yield pltpu.make_async_remote_copy(
                    src_ref=src, dst_ref=dst.at[me_t], send_sem=w_send.at[k, d], recv_sem=w_recv.at[k, d],
                    device_id=tps[d], device_id_type=MESH,
                )
        for k, (src, dst) in enumerate(((w_any, w_all), (wo_any, wo_all))):
            yield pltpu.make_async_copy(src, dst.at[me_t], w_local.at[k])

    @pl.when(step == 0)
    def _():
        barrier = pltpu.get_barrier_semaphore()
        for peer in [partner] + chips[1:] + tps[1:]:
            pl.semaphore_signal(barrier, inc=1, device_id=peer, device_id_type=MESH)
        pl.semaphore_wait(barrier, n_chip + n_tp - 1)
        for copy in weight_copies():
            copy.start()
        for e in range(3):
            w_s[:, e * cols : (e + 1) * cols] = w_ref[e]
        w_s[:, 3 * cols :] = wo_ref[...].T
        qk_s[...] = jnp.zeros_like(qk_s)
        dv_s[...] = jnp.zeros_like(dv_s)

    sub = u_s.shape[1]
    n_sub = x_ref.shape[0] // sub
    gamma, beta = gamma_ref[...], beta_ref[...]

    def norm(s):
        u_s[s % 2] = layer_norm(x_ref[s * sub : (s + 1) * sub].astype(F32), gamma, beta)[2]

    def sums(s):
        u = u_s[s % 2]
        qk = dot(u, w_s[:, : 2 * cols]).astype(BF16)
        v = dot(u, w_s[:, 2 * cols : 3 * cols]).astype(BF16)
        dout = dot(g_ref[s * sub : (s + 1) * sub], w_s[:, 3 * cols :]).astype(BF16)
        qk_s[...] += dot_rows(qk, qk)
        dv_s[...] += dot_rows(dout, v)

    norm(0)
    for s in range(n_sub):
        if s + 1 < n_sub:
            norm(s + 1)
        sums(s)

    @pl.when(step == pl.num_programs(0) - 1)
    def _():
        lane = lax.broadcasted_iota(jnp.int32, (hd, cols), 1)
        first = lane < hd
        eye = lax.broadcasted_iota(jnp.int32, (cols, cols), 0) == lax.broadcasted_iota(jnp.int32, (cols, cols), 1)

        def fold(block):
            return jnp.where(first, block[:hd], block[hd:])

        def diag_row(block):
            return jnp.sum(jnp.where(eye, block, 0.0), axis=0, keepdims=True)

        pair[0, :hd] = fold(qk_s[:cols, cols:])
        pair[0, hd : 2 * hd] = fold(dv_s[...])
        pair[0, 2 * hd :] = jnp.concatenate(
            [diag_row(qk_s[:cols, :cols]), diag_row(qk_s[cols:, cols:]), jnp.zeros((6, cols), F32)], axis=0
        )
        copy = pltpu.make_async_remote_copy(
            src_ref=pair.at[0], dst_ref=pair.at[1], send_sem=pair_send, recv_sem=pair_recv,
            device_id=partner, device_id_type=MESH,
        )
        copy.start()
        copy.wait()
        gath[0] = pair[0] + pair[1]
        copies = []
        for d in range(1, n_chip):
            copy = pltpu.make_async_remote_copy(
                src_ref=gath.at[0], dst_ref=gath.at[d], send_sem=sp_send.at[d], recv_sem=sp_recv.at[d],
                device_id=chips[d], device_id_type=MESH,
            )
            copy.start()
            copies.append(copy)
        for copy in copies:
            copy.wait()
        total = gath[chip]
        for c in range(1, n_chip):
            total = total + gath[lax.rem(chip - c + n_chip, n_chip)]

        gram, d_attn = total[:hd], total[hd : 2 * hd]
        q_row, k_row = total[2 * hd : 2 * hd + 1], total[2 * hd + 1 : 2 * hd + 2]
        q_all = jnp.sum(jnp.where(eye, jnp.broadcast_to(q_row, (cols, cols)), 0.0), axis=1, keepdims=True)
        q_col = jnp.where(first, jnp.broadcast_to(q_all[:hd], (hd, cols)), jnp.broadcast_to(q_all[hd:], (hd, cols)))
        temp = jnp.where(first, temp_ref[2 * me_t], temp_ref[2 * me_t + 1])

        def per_head(value, reduce, other):
            lo = reduce(jnp.where(first, value, other), axis=1, keepdims=True)
            hi = reduce(jnp.where(first, other, value), axis=1, keepdims=True)
            return jnp.where(first, jnp.broadcast_to(lo, (hd, cols)), jnp.broadcast_to(hi, (hd, cols)))

        norm_prod = jnp.sqrt(q_col) * jnp.sqrt(k_row)
        gram_n = gram / norm_prod
        logit = temp * gram_n
        expo = jnp.exp(logit - per_head(logit, jnp.max, -jnp.inf))
        attn = expo / per_head(expo, jnp.sum, 0.0)
        d_logit = attn * (d_attn - per_head(attn * d_attn, jnp.sum, 0.0))
        temp_part = jnp.sum(per_head(d_logit * gram_n, jnp.sum, 0.0), axis=0, keepdims=True)
        grad_sn = temp * d_logit
        prod = grad_sn * gram_n
        same = lax.broadcasted_iota(jnp.int32, (hd, cols), 0) == lax.rem(lane, hd)
        q_coef = jnp.sum(jnp.where(same, -per_head(prod, jnp.sum, 0.0) / q_col, 0.0), axis=0, keepdims=True)
        k_coef = -jnp.sum(prod, axis=0, keepdims=True) / k_row

        mats[0, :hd] = attn.astype(BF16)
        mats[0, hd:] = (grad_sn / norm_prod).astype(BF16)
        rows[0] = jnp.concatenate([q_coef, k_coef, temp_part, jnp.zeros((5, cols), F32)], axis=0)
        copies = []
        for d in range(1, n_tp):
            for k, ref in enumerate((mats, rows)):
                copy = pltpu.make_async_remote_copy(
                    src_ref=ref.at[0], dst_ref=ref.at[d], send_sem=tp_send.at[k, d], recv_sem=tp_recv.at[k, d],
                    device_id=tps[d], device_id_type=MESH,
                )
                copy.start()
                copies.append(copy)
        for copy in copies:
            copy.wait()
        for t in range(n_tp):
            slot = lax.rem(me_t - t + n_tp, n_tp)
            mats_ref[t] = mats[slot]
            part = rows[slot]
            rows_ref[t] = part
            gt_ref[2 * t] = part[2, 0]
            gt_ref[2 * t + 1] = part[2, hd]
        for copy in weight_copies():
            copy.wait()


def run_state(n_sp, n_tp, x, g, w, wo, gamma, beta, temp):
    tokens, width = x.shape
    cols = wo.shape[0]
    r, sub = STATS_ROWS, STATS_SUB
    tile = pl.BlockSpec((r, width), lambda i: (i, 0))

    def whole(shape):
        return pl.BlockSpec(shape, lambda i: (0,) * len(shape))

    hbm = pl.BlockSpec(memory_space=pl.ANY)
    smem = pl.BlockSpec(memory_space=pltpu.SMEM)
    vmem, dma = pltpu.VMEM, pltpu.SemaphoreType.DMA
    return pl.pallas_call(
        functools.partial(state_kernel, n_sp, n_tp),
        grid=(tokens // r,),
        out_shape=(
            jax.ShapeDtypeStruct((n_tp,) + w.shape, BF16),
            jax.ShapeDtypeStruct((n_tp,) + wo.shape, BF16),
            jax.ShapeDtypeStruct((n_tp, cols, cols), BF16),
            jax.ShapeDtypeStruct((n_tp, 8, cols), F32),
            jax.ShapeDtypeStruct(temp.shape, F32),
        ),
        in_specs=[tile, tile, whole(w.shape), whole(wo.shape), whole((1, width)), whole((1, width)), smem, hbm, hbm],
        out_specs=(hbm, hbm, whole((n_tp, cols, cols)), whole((n_tp, 8, cols)), smem),
        scratch_shapes=[
            vmem((width, 4 * cols), BF16), vmem((2, sub, width), BF16),
            vmem((2 * cols, 2 * cols), F32), vmem((cols, cols), F32),
            vmem((2, cols + 8, cols), F32), vmem((n_sp // 2, cols + 8, cols), F32),
            vmem((n_tp, cols, cols), BF16), vmem((n_tp, 8, cols), F32),
            dma((2, n_tp)), dma((2, n_tp)), dma((2,)), dma, dma, dma((n_sp // 2,)), dma((n_sp // 2,)),
            dma((2, n_tp)), dma((2, n_tp)),
        ],
        compiler_params=pltpu.CompilerParams(
            dimension_semantics=("arbitrary",), vmem_limit_bytes=48 << 20, collective_id=0, has_side_effects=True
        ),
        name="state",
    )(x, g, w, wo, gamma, beta, temp, w, wo)


def main_kernel(
    n_tp, t_ref, x_ref, g_ref, w_ref, wo_ref, mats_ref, rows_ref, gamma_ref, beta_ref,
    y_ref, dx_ref, dw_ref, dwo_ref, dgb_ref,
    w_s, wt_s, wo_s, wot_s, at_s, a_s, gt_s, g_s, co_s, u_s, r_s, o_s, own_s, xh_s, du_s, dwt_s,
):
    width = x_ref.shape[1]
    cols = width // n_tp
    hd = cols // 2
    me_t = t_ref[0]
    step = pl.program_id(0)

    @pl.when(step == 0)
    def _():
        for t in range(n_tp):
            at = t * cols
            for e in range(3):
                w_s[:, e * width + at : e * width + at + cols] = w_ref[t, e]
                wt_s[e * width + at : e * width + at + cols, :] = w_ref[t, e].T
            wo_s[at : at + cols, :] = wo_ref[t]
            wot_s[:, at : at + cols] = wo_ref[t].T
        for ref in (at_s, a_s, gt_s, g_s):
            ref[...] = jnp.zeros_like(ref)
        first = lax.broadcasted_iota(jnp.int32, (hd, cols), 1) < hd
        for t in range(n_tp):
            p, off = t // 2, (t % 2) * cols
            for k, (plain, trans) in enumerate(((a_s, at_s), (g_s, gt_s))):
                block = mats_ref[t, k * hd : (k + 1) * hd].astype(F32)
                full = jnp.concatenate([jnp.where(first, block, 0.0), jnp.where(first, 0.0, block)], axis=0)
                plain[p, off : off + cols, off : off + cols] = full.astype(BF16)
                trans[p, off : off + cols, off : off + cols] = full.T.astype(BF16)
            co_s[0:1, t * cols : (t + 1) * cols] = rows_ref[t, 0:1]
            co_s[1:2, t * cols : (t + 1) * cols] = rows_ref[t, 1:2]
        dwt_s[...] = jnp.zeros_like(dwt_s)
        dwo_ref[...] = jnp.zeros_like(dwo_ref)
        dgb_ref[...] = jnp.zeros_like(dgb_ref)

    sub = u_s.shape[1]
    n_sub = x_ref.shape[0] // sub
    gamma, beta = gamma_ref[...], beta_ref[...]
    mine = pl.multiple_of(me_t * cols, cols)

    def norm(s):
        x_hat, inv_std, u = layer_norm(x_ref[s * sub : (s + 1) * sub].astype(F32), gamma, beta)
        xh_s[s % 2] = x_hat
        u_s[s % 2] = u
        return inv_std

    def attend(s):
        b, at = s % 2, slice(s * sub, (s + 1) * sub)
        for p in range(2):
            lo, hi = p * 2 * cols, (p + 1) * 2 * cols
            q = dot(u_s[b], w_s[:, lo:hi]).astype(BF16)
            k = dot(u_s[b], w_s[:, width + lo : width + hi]).astype(BF16)
            v = dot(u_s[b], w_s[:, 2 * width + lo : 2 * width + hi]).astype(BF16)
            dout = dot(g_ref[at], wot_s[:, lo:hi]).astype(BF16)
            o_s[b, :, lo:hi] = dot(v, at_s[p]).astype(BF16)
            r_s[b, :, 2 * width + lo : 2 * width + hi] = dot(dout, a_s[p]).astype(BF16)
            r_s[b, :, lo:hi] = (dot(k, gt_s[p]) + q.astype(F32) * co_s[0:1, lo:hi]).astype(BF16)
            r_s[b, :, width + lo : width + hi] = (dot(q, g_s[p]) + k.astype(F32) * co_s[1:2, lo:hi]).astype(BF16)
        y_ref[at] = (x_ref[at].astype(F32) + dot(o_s[b], wo_s[...])).astype(BF16)
        du_s[b] = dot(r_s[b], wt_s[...])

    def weights(s):
        b, at = s % 2, slice(s * sub, (s + 1) * sub)
        for e in range(3):
            own_s[b, :, e * cols : (e + 1) * cols] = r_s[b, :, pl.ds(e * width + mine, cols)]
        dwt_s[...] += dot_rows(own_s[b], u_s[b])
        dwo_ref[...] += dot_rows(o_s[b, :, pl.ds(mine, cols)], g_ref[at])

    def norm_grad(s, inv_std):
        b, at = s % 2, slice(s * sub, (s + 1) * sub)
        du, x_hat = du_s[b], xh_s[b]
        dgb_ref[0:1] += jnp.sum(du * x_hat, axis=0, keepdims=True)
        dgb_ref[1:2] += jnp.sum(du, axis=0, keepdims=True)
        gx = du * gamma
        mean1 = jnp.mean(gx, axis=-1, keepdims=True)
        mean2 = jnp.mean(gx * x_hat, axis=-1, keepdims=True)
        dx_ref[at] = (g_ref[at].astype(F32) + inv_std * (gx - mean1 - x_hat * mean2)).astype(BF16)

    inv = {0: norm(0)}
    for s in range(n_sub):
        if s + 1 < n_sub:
            inv[s + 1] = norm(s + 1)
        attend(s)
        norm_grad(s, inv[s])
        weights(s)

    @pl.when(step == pl.num_programs(0) - 1)
    def _():
        for e in range(3):
            dw_ref[:, e * cols : (e + 1) * cols] = dwt_s[e * cols : (e + 1) * cols, :].T


def run_main(n_tp, me_t, x, g, w, wo, mats, rows, gamma, beta):
    tokens, width = x.shape
    cols = width // n_tp
    r, sub = MAIN_ROWS, MAIN_SUB
    tile = pl.BlockSpec((r, width), lambda i, t: (i, 0))

    def whole(shape):
        return pl.BlockSpec(shape, lambda i, t: (0,) * len(shape))

    vmem = pltpu.VMEM
    pair = (2, 2 * cols, 2 * cols)
    return pl.pallas_call(
        functools.partial(main_kernel, n_tp),
        grid_spec=pltpu.PrefetchScalarGridSpec(
            num_scalar_prefetch=1,
            grid=(tokens // r,),
            in_specs=[tile, tile] + [whole(a.shape) for a in (w, wo, mats, rows, gamma, beta)],
            out_specs=(tile, tile, whole((width, 3 * cols)), whole((cols, width)), whole((8, width))),
            scratch_shapes=[
                vmem((width, 3 * width), BF16), vmem((3 * width, width), BF16),
                vmem((width, width), BF16), vmem((width, width), BF16),
                vmem(pair, BF16), vmem(pair, BF16), vmem(pair, BF16), vmem(pair, BF16),
                vmem((8, width), F32),
                vmem((2, sub, width), BF16), vmem((2, sub, 3 * width), BF16),
                vmem((2, sub, width), BF16), vmem((2, sub, 3 * cols), BF16),
                vmem((2, sub, width), F32), vmem((2, sub, width), F32),
                vmem((3 * cols, width), F32),
            ],
        ),
        out_shape=(
            jax.ShapeDtypeStruct(x.shape, BF16),
            jax.ShapeDtypeStruct(x.shape, BF16),
            jax.ShapeDtypeStruct((width, 3 * cols), F32),
            jax.ShapeDtypeStruct((cols, width), F32),
            jax.ShapeDtypeStruct((8, width), F32),
        ),
        compiler_params=pltpu.CompilerParams(dimension_semantics=("arbitrary",), vmem_limit_bytes=60 << 20),
        cost_estimate=pl.CostEstimate(
            flops=2 * tokens * width * width * 11, bytes_accessed=8 * tokens * width, transcendentals=0
        ),
        name="main",
    )(me_t, x, g, w, wo, mats, rows, gamma, beta)


def reduce_kernel(
    n_chip, dw_ref, dwo_ref, dgb_ref, dw_out, dwo_out, g_out,
    got_w, got_o, sum_w, sum_o, via_w, via_o, in_w, in_o, gam, in_g,
    a_send, a_recv, g_send, g_recv, b_send, b_recv,
):
    me = lax.axis_index("sp")
    core, chip = lax.rem(me, 2), me // 2
    partner = {"sp": me + 1 - 2 * core}
    right, far, left = (lax.rem(chip + d, n_chip) for d in range(1, n_chip))
    peers = [None] + [{"sp": 2 * c + core} for c in (right, far, left)]
    barrier = pltpu.get_barrier_semaphore()
    for peer in [partner] + peers[1:]:
        pl.semaphore_signal(barrier, inc=1, device_id=peer, device_id_type=MESH)
    for c in range(4):
        gam[0, c : c + 1] = dgb_ref[0:1, c * 128 : (c + 1) * 128]
        gam[0, 4 + c : 5 + c] = dgb_ref[1:2, c * 128 : (c + 1) * 128]
    pl.semaphore_wait(barrier, n_chip)

    def remote(src, dst, send, recv, peer):
        copy = pltpu.make_async_remote_copy(
            src_ref=src, dst_ref=dst, send_sem=send, recv_sem=recv, device_id=peer, device_id_type=MESH
        )
        copy.start()
        return copy

    w_copy = remote(dw_ref.at[:, 1 - core], got_w, a_send.at[0], a_recv.at[0], partner)
    o_copy = remote(dwo_ref.at[:, 1 - core], got_o, a_send.at[1], a_recv.at[1], partner)
    g_copy = remote(gam.at[0], gam.at[1], a_send.at[2], a_recv.at[2], partner)
    w_copy.wait()
    o_copy.wait()
    sum_w[...] = dw_ref[:, core] + got_w[...]
    sum_o[...] = dwo_ref[:, core] + got_o[...]
    hw, ho = sum_w.shape[1] // 2, sum_o.shape[1] // 2
    w_half, o_half = (pl.ds(0, hw), pl.ds(hw, hw)), (pl.ds(0, ho), pl.ds(ho, ho))

    via, near, last = [], [], []
    for h, peer in ((0, peers[1]), (1, peers[3])):
        via.append(remote(sum_w.at[far, w_half[h]], via_w.at[h], b_send.at[0, h], b_recv.at[0, h], peer))
        via.append(remote(sum_o.at[far, o_half[h]], via_o.at[h], b_send.at[1, h], b_recv.at[1, h], peer))
    for h, to, peer in ((0, right, peers[1]), (1, left, peers[3])):
        o = 1 - h
        near.append(remote(sum_w.at[to, w_half[o]], in_w.at[h, w_half[o]], b_send.at[2, h], b_recv.at[2, h], peer))
        near.append(remote(sum_o.at[to, o_half[o]], in_o.at[h, o_half[o]], b_send.at[3, h], b_recv.at[3, h], peer))
    g_copy.wait()
    in_g[0] = gam[0] + gam[1]
    for d in range(1, n_chip):
        near.append(remote(in_g.at[0], in_g.at[d], g_send.at[d], g_recv.at[d], peers[d]))
    for h, to, peer in ((0, right, peers[1]), (1, left, peers[3])):
        via[2 * h].wait()
        via[2 * h + 1].wait()
        sum_w[to, w_half[h]] += via_w[h]
        sum_o[to, o_half[h]] += via_o[h]
        last.append(remote(sum_w.at[to, w_half[h]], in_w.at[h, w_half[h]], b_send.at[4, h], b_recv.at[4, h], peer))
        last.append(remote(sum_o.at[to, o_half[h]], in_o.at[h, o_half[h]], b_send.at[5, h], b_recv.at[5, h], peer))
    for copy in near + last:
        copy.wait()
    w_tot = sum_w[chip] + in_w[0] + in_w[1]
    cols = dw_out.shape[2]
    for e in range(3):
        dw_out[e] = w_tot[:, e * cols : (e + 1) * cols]
    dwo_out[...] = sum_o[chip] + in_o[0] + in_o[1]
    g_tot = in_g[chip]
    for c in range(1, n_chip):
        g_tot = g_tot + in_g[lax.rem(chip - c + n_chip, n_chip)]
    g_out[...] = g_tot


def finish_kernel(dw_ref, dwo_ref, g_ref, gt_ref, dw_out, dwo_out, dg_out, db_out, gt_out):
    dw_out[...] = dw_ref[...]
    dwo_out[...] = dwo_ref[...]
    for c in range(4):
        dg_out[0:1, c * 128 : (c + 1) * 128] = g_ref[c : c + 1]
        db_out[0:1, c * 128 : (c + 1) * 128] = g_ref[4 + c : 5 + c]
    for h in range(gt_ref.shape[0]):
        gt_out[h] = gt_ref[h]


def run_reduce(n_sp, dw, dwo, dgb, grad_temp):
    width, cols3 = dw.shape
    cols = dwo.shape[0]
    n_chip = n_sp // 2
    assert n_chip == 4 and width == 512
    dw = dw.reshape(n_chip, 2, width // n_sp, cols3)
    dwo = dwo.reshape(n_chip, 2, cols // n_sp, width)
    w_shape, o_shape = dw.shape[2:], dwo.shape[2:]
    w_half, o_half = (w_shape[0] // 2, w_shape[1]), (o_shape[0] // 2, o_shape[1])
    spec = pl.BlockSpec(memory_space=pltpu.VMEM)
    smem = pl.BlockSpec(memory_space=pltpu.SMEM)
    vmem, dma = pltpu.VMEM, pltpu.SemaphoreType.DMA
    results = (
        jax.ShapeDtypeStruct((3, width // n_sp, cols3 // 3), F32),
        jax.ShapeDtypeStruct((cols // n_sp, width), F32),
    )
    dw, dwo, g = pl.pallas_call(
        functools.partial(reduce_kernel, n_chip),
        out_shape=results + (jax.ShapeDtypeStruct((8, 128), F32),),
        in_specs=[spec] * 3,
        out_specs=(spec,) * 3,
        scratch_shapes=[
            vmem((n_chip,) + w_shape, F32), vmem((n_chip,) + o_shape, F32),
            vmem((n_chip,) + w_shape, F32), vmem((n_chip,) + o_shape, F32),
            vmem((2,) + w_half, F32), vmem((2,) + o_half, F32),
            vmem((2,) + w_shape, F32), vmem((2,) + o_shape, F32),
            vmem((2, 8, 128), F32), vmem((n_chip, 8, 128), F32),
            dma((3,)), dma((3,)), dma((n_chip,)), dma((n_chip,)), dma((6, 2)), dma((6, 2)),
        ],
        compiler_params=pltpu.CompilerParams(collective_id=1, has_side_effects=True),
        name="reduce",
    )(dw, dwo, dgb)
    row = jax.ShapeDtypeStruct((1, width), F32)
    return pl.pallas_call(
        finish_kernel,
        out_shape=results + (row, row, jax.ShapeDtypeStruct(grad_temp.shape, F32)),
        in_specs=[spec] * 3 + [smem],
        out_specs=(spec,) * 4 + (smem,),
        name="finish",
    )(dw, dwo, g, grad_temp)


def solution(mesh):
    n_tp, n_sp = mesh.shape["tp"], mesh.shape["sp"]
    row_spec = P(("dp", "sp"), None)

    def local_step(x, g, w_qkv, w_out, ln_gamma, ln_beta, temperature):
        width = x.shape[1]
        gamma, beta = ln_gamma.reshape(1, width), ln_beta.reshape(1, width)
        me_t = lax.axis_index("tp").astype(jnp.int32).reshape(1)
        w, wo, mats, rows, grad_temp = run_state(
            n_sp, n_tp, x, g, w_qkv.transpose(1, 0, 2), w_out, gamma, beta, temperature
        )
        y, dx, dw, dwo, dgb = run_main(n_tp, me_t, x, g, w, wo, mats, rows, gamma, beta)
        dw, dwo, dgamma, dbeta, grad_temp = run_reduce(n_sp, dw, dwo, dgb, grad_temp)
        return y, dx, dw.transpose(1, 0, 2), dwo, dgamma.reshape(-1), dbeta.reshape(-1), grad_temp

    in_specs = (row_spec, row_spec, P(None, None, "tp"), P("tp", None), P(None), P(None), P(None))
    out_specs = (row_spec, row_spec, P(("dp", "sp"), None, "tp"), P(("dp", "tp", "sp"), None), P("dp"), P("dp"), P("dp"))
    return jax.shard_map(local_step, mesh=mesh, in_specs=in_specs, out_specs=out_specs, check_vma=False)
```

```python
import functools

import jax
import jax.numpy as jnp
from jax import lax
from jax.experimental import pallas as pl
from jax.experimental.pallas import tpu as pltpu
from jax.sharding import PartitionSpec as P

LN_EPS = 1e-6
F32 = jnp.float32
BF16 = jnp.bfloat16
MESH = pl.DeviceIdType.MESH
STATS_ROWS = 2048
STATS_SUB = 512
CHUNK = 128
MAIN_ROWS = 2048
MAIN_SUB = 512


def dot(lhs, rhs):
    return jnp.dot(lhs, rhs, preferred_element_type=F32)


def dot_rows(lhs, rhs):
    return lax.dot_general(lhs, rhs, (((0,), (0,)), ((), ())), preferred_element_type=F32)


def dot_cols(lhs, rhs):
    return lax.dot_general(lhs, rhs, (((1,), (1,)), ((), ())), preferred_element_type=F32)


def layer_norm(x, gamma, beta):
    centered = x - jnp.mean(x, axis=-1, keepdims=True)
    inv_std = lax.rsqrt(jnp.mean(centered * centered, axis=-1, keepdims=True) + LN_EPS)
    x_hat = centered * inv_std
    return x_hat, inv_std, (x_hat * gamma + beta).astype(BF16)


def weave(steps, *sides):
    order = [((i + 0.5) / len(steps), 0, i, f) for i, f in enumerate(steps)]
    for n, side in enumerate(sides):
        order += [((i + 0.25) / len(side), n + 1, i, f) for i, f in enumerate(side)]
    for *_, f in sorted(order, key=lambda e: e[:3]):
        f()


def state_kernel(
    n_sp, n_tp, x_ref, g_ref, w_ref, wo_ref, gamma_ref, beta_ref, temp_ref, w_any, wo_any,
    w_all, wo_all, mats_ref, rows_ref, gt_ref,
    wt_s, wot_s, u_s, qk_s, vd_s, pair, gath, mats, rows,
    w_send, w_recv, p_send, p_recv, w_local, pair_send, pair_recv, sp_send, sp_recv, tp_send, tp_recv,
):
    step = pl.program_id(0)
    me_s, me_t = lax.axis_index("sp"), lax.axis_index("tp")
    n_chip = n_sp // 2
    core, chip = lax.rem(me_s, 2), me_s // 2
    cols, width = wo_ref.shape
    hd = cols // 2
    partner = {"sp": me_s + 1 - 2 * core}
    chips = [{"sp": 2 * lax.rem(chip + d, n_chip) + core} for d in range(n_chip)]
    tps = [{"tp": lax.rem(me_t + d, n_tp)} for d in range(n_tp)]

    n_rows, n_wo = w_any.shape[1] // 2, wo_any.shape[0] // 2
    rows_of = pl.ds(pl.multiple_of(core * n_rows, n_rows), n_rows)
    wo_of = pl.ds(pl.multiple_of(core * n_wo, n_wo), n_wo)

    def gather_copies():
        copies = []
        for d in range(1, n_tp):
            for k, (src, dst) in enumerate(
                ((w_any.at[:, rows_of], w_all.at[me_t, :, rows_of]), (wo_any.at[wo_of], wo_all.at[me_t, wo_of]))
            ):
                copies.append(pltpu.make_async_remote_copy(
                    src_ref=src, dst_ref=dst, send_sem=w_send.at[k, d], recv_sem=w_recv.at[k, d],
                    device_id=tps[d], device_id_type=MESH,
                ))
        return copies

    def pass_copies():
        copies = []
        for d in range(1, n_tp):
            t = lax.rem(me_t - d + n_tp, n_tp)
            for k, ref in enumerate((w_all.at[t, :, rows_of], wo_all.at[t, wo_of])):
                copies.append(pltpu.make_async_remote_copy(
                    src_ref=ref, dst_ref=ref, send_sem=p_send.at[k, d], recv_sem=p_recv.at[k, d],
                    device_id=partner, device_id_type=MESH,
                ))
        return copies

    def local_copies():
        return [
            pltpu.make_async_copy(src, dst.at[me_t], w_local.at[k])
            for k, (src, dst) in enumerate(((w_any, w_all), (wo_any, wo_all)))
        ]

    @pl.when(step == 0)
    def _():
        barrier = pltpu.get_barrier_semaphore()
        for peer in [partner] + chips[1:] + tps[1:]:
            pl.semaphore_signal(barrier, inc=1, device_id=peer, device_id_type=MESH)
        pl.semaphore_wait(barrier, n_chip + n_tp - 1)
        for copy in gather_copies() + local_copies():
            copy.start()
        for e in range(3):
            wt_s[e * cols : (e + 1) * cols, :] = w_ref[e].T
        wot_s[...] = wo_ref[...].T
        qk_s[...] = jnp.zeros_like(qk_s)
        vd_s[...] = jnp.zeros_like(vd_s)

    @pl.when(step == pl.num_programs(0) - 1)
    def _():
        for copy in gather_copies():
            copy.wait()
        for copy in pass_copies():
            copy.start()

    sub = u_s.shape[1]
    n_sub = x_ref.shape[0] // sub
    gamma, beta = gamma_ref[...], beta_ref[...]

    def norm(s):
        def piece(at):
            x = x_ref[s * sub + at : s * sub + at + CHUNK].astype(F32)
            u_s[s % 2, at : at + CHUNK] = layer_norm(x, gamma, beta)[2]

        return [functools.partial(piece, at) for at in range(0, sub, CHUNK)]

    def sums(s):
        qkv = dot_cols(wt_s[...], u_s[s % 2]).astype(BF16)
        qk_s[...] += dot_cols(qkv[: 2 * cols], qkv[: 2 * cols])
        dout = dot(g_ref[s * sub : (s + 1) * sub], wot_s[...]).astype(BF16)
        vd_s[...] += dot(qkv[2 * cols :], dout)

    weave(norm(0))
    for s in range(n_sub):
        if s + 1 < n_sub:
            weave(norm(s + 1))
        sums(s)

    @pl.when(step == pl.num_programs(0) - 1)
    def _():
        lane = lax.broadcasted_iota(jnp.int32, (hd, cols), 1)
        first = lane < hd
        eye = lax.broadcasted_iota(jnp.int32, (cols, cols), 0) == lax.broadcasted_iota(jnp.int32, (cols, cols), 1)

        def fold(block):
            return jnp.where(first, block[:hd], block[hd:])

        def diag_row(block):
            return jnp.sum(jnp.where(eye, block, 0.0), axis=0, keepdims=True)

        pair[0, :hd] = fold(qk_s[:cols, cols:])
        pair[0, hd : 2 * hd] = fold(vd_s[...].T)
        pair[0, 2 * hd :] = jnp.concatenate(
            [diag_row(qk_s[:cols, :cols]), diag_row(qk_s[cols:, cols:]), jnp.zeros((6, cols), F32)], axis=0
        )
        copy = pltpu.make_async_remote_copy(
            src_ref=pair.at[0], dst_ref=pair.at[1], send_sem=pair_send, recv_sem=pair_recv,
            device_id=partner, device_id_type=MESH,
        )
        copy.start()
        copy.wait()
        gath[0] = pair[0] + pair[1]
        copies = []
        for d in range(1, n_chip):
            copy = pltpu.make_async_remote_copy(
                src_ref=gath.at[0], dst_ref=gath.at[d], send_sem=sp_send.at[d], recv_sem=sp_recv.at[d],
                device_id=chips[d], device_id_type=MESH,
            )
            copy.start()
            copies.append(copy)
        for copy in copies:
            copy.wait()
        total = gath[chip]
        for c in range(1, n_chip):
            total = total + gath[lax.rem(chip - c + n_chip, n_chip)]

        gram, d_attn = total[:hd], total[hd : 2 * hd]
        q_row, k_row = total[2 * hd : 2 * hd + 1], total[2 * hd + 1 : 2 * hd + 2]
        q_all = jnp.sum(jnp.where(eye, jnp.broadcast_to(q_row, (cols, cols)), 0.0), axis=1, keepdims=True)
        q_col = jnp.where(first, jnp.broadcast_to(q_all[:hd], (hd, cols)), jnp.broadcast_to(q_all[hd:], (hd, cols)))
        temp = jnp.where(first, temp_ref[2 * me_t], temp_ref[2 * me_t + 1])

        def per_head(value, reduce, other):
            lo = reduce(jnp.where(first, value, other), axis=1, keepdims=True)
            hi = reduce(jnp.where(first, other, value), axis=1, keepdims=True)
            return jnp.where(first, jnp.broadcast_to(lo, (hd, cols)), jnp.broadcast_to(hi, (hd, cols)))

        norm_prod = jnp.sqrt(q_col) * jnp.sqrt(k_row)
        gram_n = gram / norm_prod
        logit = temp * gram_n
        expo = jnp.exp(logit - per_head(logit, jnp.max, -jnp.inf))
        attn = expo / per_head(expo, jnp.sum, 0.0)
        d_logit = attn * (d_attn - per_head(attn * d_attn, jnp.sum, 0.0))
        temp_part = jnp.sum(per_head(d_logit * gram_n, jnp.sum, 0.0), axis=0, keepdims=True)
        grad_sn = temp * d_logit
        prod = grad_sn * gram_n
        same = lax.broadcasted_iota(jnp.int32, (hd, cols), 0) == lax.rem(lane, hd)
        q_coef = jnp.sum(jnp.where(same, -per_head(prod, jnp.sum, 0.0) / q_col, 0.0), axis=0, keepdims=True)
        k_coef = -jnp.sum(prod, axis=0, keepdims=True) / k_row

        mats[0, :hd] = attn.astype(BF16)
        mats[0, hd:] = (grad_sn / norm_prod).astype(BF16)
        rows[0] = jnp.concatenate([q_coef, k_coef, temp_part, jnp.zeros((5, cols), F32)], axis=0)
        copies = []
        for d in range(1, n_tp):
            for k, ref in enumerate((mats, rows)):
                copy = pltpu.make_async_remote_copy(
                    src_ref=ref.at[0], dst_ref=ref.at[d], send_sem=tp_send.at[k, d], recv_sem=tp_recv.at[k, d],
                    device_id=tps[d], device_id_type=MESH,
                )
                copy.start()
                copies.append(copy)
        for copy in copies:
            copy.wait()
        for t in range(n_tp):
            slot = lax.rem(me_t - t + n_tp, n_tp)
            mats_ref[t] = mats[slot]
            part = rows[slot]
            rows_ref[t] = part
            gt_ref[2 * t] = part[2, 0]
            gt_ref[2 * t + 1] = part[2, hd]
        for copy in pass_copies() + local_copies():
            copy.wait()


def run_state(n_sp, n_tp, x, g, w, wo, gamma, beta, temp):
    tokens, width = x.shape
    cols = wo.shape[0]
    r, sub = STATS_ROWS, STATS_SUB
    tile = pl.BlockSpec((r, width), lambda i: (i, 0))

    def whole(shape):
        return pl.BlockSpec(shape, lambda i: (0,) * len(shape))

    hbm = pl.BlockSpec(memory_space=pl.ANY)
    smem = pl.BlockSpec(memory_space=pltpu.SMEM)
    vmem, dma = pltpu.VMEM, pltpu.SemaphoreType.DMA
    return pl.pallas_call(
        functools.partial(state_kernel, n_sp, n_tp),
        grid=(tokens // r,),
        out_shape=(
            jax.ShapeDtypeStruct((n_tp,) + w.shape, BF16),
            jax.ShapeDtypeStruct((n_tp,) + wo.shape, BF16),
            jax.ShapeDtypeStruct((n_tp, cols, cols), BF16),
            jax.ShapeDtypeStruct((n_tp, 8, cols), F32),
            jax.ShapeDtypeStruct(temp.shape, F32),
        ),
        in_specs=[tile, tile, whole(w.shape), whole(wo.shape), whole((1, width)), whole((1, width)), smem, hbm, hbm],
        out_specs=(hbm, hbm, whole((n_tp, cols, cols)), whole((n_tp, 8, cols)), smem),
        scratch_shapes=[
            vmem((3 * cols, width), BF16), vmem((width, cols), BF16), vmem((2, sub, width), BF16),
            vmem((2 * cols, 2 * cols), F32), vmem((cols, cols), F32),
            vmem((2, cols + 8, cols), F32), vmem((n_sp // 2, cols + 8, cols), F32),
            vmem((n_tp, cols, cols), BF16), vmem((n_tp, 8, cols), F32),
            dma((2, n_tp)), dma((2, n_tp)), dma((2, n_tp)), dma((2, n_tp)), dma((2,)), dma, dma, dma((n_sp // 2,)), dma((n_sp // 2,)),
            dma((2, n_tp)), dma((2, n_tp)),
        ],
        compiler_params=pltpu.CompilerParams(
            dimension_semantics=("arbitrary",), vmem_limit_bytes=60 << 20, collective_id=0, has_side_effects=True
        ),
        name="state",
    )(x, g, w, wo, gamma, beta, temp, w, wo)


def main_kernel(
    n_tp, t_ref, x_ref, g_ref, w_ref, wo_ref, mats_ref, rows_ref, gamma_ref, beta_ref,
    y_ref, dx_ref, dw_ref, dwo_ref, dgb_ref,
    w_s, wt_s, wo_s, wot_s, at_s, a_s, gt_s, g_s, co_s, u_s, r_s, o_s, own_s, xh_s, du_s, dwt_s,
):
    width = x_ref.shape[1]
    cols = width // n_tp
    hd = cols // 2
    me_t = t_ref[0]
    step = pl.program_id(0)

    @pl.when(step == 0)
    def _():
        for t in range(n_tp):
            at = t * cols
            for e in range(3):
                w_s[:, e * width + at : e * width + at + cols] = w_ref[t, e]
                wt_s[e * width + at : e * width + at + cols, :] = w_ref[t, e].T
            wo_s[at : at + cols, :] = wo_ref[t]
            wot_s[:, at : at + cols] = wo_ref[t].T
        for ref in (at_s, a_s, gt_s, g_s):
            ref[...] = jnp.zeros_like(ref)
        first = lax.broadcasted_iota(jnp.int32, (hd, cols), 1) < hd
        for t in range(n_tp):
            p, off = t // 2, (t % 2) * cols
            for k, (plain, trans) in enumerate(((a_s, at_s), (g_s, gt_s))):
                block = mats_ref[t, k * hd : (k + 1) * hd].astype(F32)
                full = jnp.concatenate([jnp.where(first, block, 0.0), jnp.where(first, 0.0, block)], axis=0)
                plain[p, off : off + cols, off : off + cols] = full.astype(BF16)
                trans[p, off : off + cols, off : off + cols] = full.T.astype(BF16)
            co_s[0:1, t * cols : (t + 1) * cols] = rows_ref[t, 0:1]
            co_s[1:2, t * cols : (t + 1) * cols] = rows_ref[t, 1:2]
        dwt_s[...] = jnp.zeros_like(dwt_s)
        dwo_ref[...] = jnp.zeros_like(dwo_ref)
        dgb_ref[...] = jnp.zeros_like(dgb_ref)

    sub = u_s.shape[1]
    n_sub = x_ref.shape[0] // sub
    gamma, beta = gamma_ref[...], beta_ref[...]
    mine = pl.multiple_of(me_t * cols, cols)

    def norm(s):
        x_hat, inv_std, u = layer_norm(x_ref[s * sub : (s + 1) * sub].astype(F32), gamma, beta)
        xh_s[s % 2] = x_hat
        u_s[s % 2] = u
        return inv_std

    def attend(s):
        b, at = s % 2, slice(s * sub, (s + 1) * sub)
        for p in range(2):
            lo, hi = p * 2 * cols, (p + 1) * 2 * cols
            q = dot(u_s[b], w_s[:, lo:hi]).astype(BF16)
            k = dot(u_s[b], w_s[:, width + lo : width + hi]).astype(BF16)
            v = dot(u_s[b], w_s[:, 2 * width + lo : 2 * width + hi]).astype(BF16)
            dout = dot(g_ref[at], wot_s[:, lo:hi]).astype(BF16)
            o_s[b, :, lo:hi] = dot(v, at_s[p]).astype(BF16)
            r_s[b, :, 2 * width + lo : 2 * width + hi] = dot(dout, a_s[p]).astype(BF16)
            r_s[b, :, lo:hi] = (dot(k, gt_s[p]) + q.astype(F32) * co_s[0:1, lo:hi]).astype(BF16)
            r_s[b, :, width + lo : width + hi] = (dot(q, g_s[p]) + k.astype(F32) * co_s[1:2, lo:hi]).astype(BF16)
        y_ref[at] = (x_ref[at].astype(F32) + dot(o_s[b], wo_s[...])).astype(BF16)
        du_s[b] = dot(r_s[b], wt_s[...])

    def weights(s):
        b, at = s % 2, slice(s * sub, (s + 1) * sub)
        for e in range(3):
            own_s[b, :, e * cols : (e + 1) * cols] = r_s[b, :, pl.ds(e * width + mine, cols)]
        dwt_s[...] += dot_rows(own_s[b], u_s[b])
        dwo_ref[...] += dot_rows(o_s[b, :, pl.ds(mine, cols)], g_ref[at])

    def norm_grad(s, inv_std):
        b, at = s % 2, slice(s * sub, (s + 1) * sub)
        du, x_hat = du_s[b], xh_s[b]
        dgb_ref[0:1] += jnp.sum(du * x_hat, axis=0, keepdims=True)
        dgb_ref[1:2] += jnp.sum(du, axis=0, keepdims=True)
        gx = du * gamma
        mean1 = jnp.mean(gx, axis=-1, keepdims=True)
        mean2 = jnp.mean(gx * x_hat, axis=-1, keepdims=True)
        dx_ref[at] = (g_ref[at].astype(F32) + inv_std * (gx - mean1 - x_hat * mean2)).astype(BF16)

    inv = {0: norm(0)}
    for s in range(n_sub):
        if s + 1 < n_sub:
            inv[s + 1] = norm(s + 1)
        attend(s)
        norm_grad(s, inv[s])
        weights(s)

    @pl.when(step == pl.num_programs(0) - 1)
    def _():
        for e in range(3):
            dw_ref[:, e * cols : (e + 1) * cols] = dwt_s[e * cols : (e + 1) * cols, :].T


def run_main(n_tp, me_t, x, g, w, wo, mats, rows, gamma, beta):
    tokens, width = x.shape
    cols = width // n_tp
    r, sub = MAIN_ROWS, MAIN_SUB
    tile = pl.BlockSpec((r, width), lambda i, t: (i, 0))

    def whole(shape):
        return pl.BlockSpec(shape, lambda i, t: (0,) * len(shape))

    vmem = pltpu.VMEM
    pair = (2, 2 * cols, 2 * cols)
    return pl.pallas_call(
        functools.partial(main_kernel, n_tp),
        grid_spec=pltpu.PrefetchScalarGridSpec(
            num_scalar_prefetch=1,
            grid=(tokens // r,),
            in_specs=[tile, tile] + [whole(a.shape) for a in (w, wo, mats, rows, gamma, beta)],
            out_specs=(tile, tile, whole((width, 3 * cols)), whole((cols, width)), whole((8, width))),
            scratch_shapes=[
                vmem((width, 3 * width), BF16), vmem((3 * width, width), BF16),
                vmem((width, width), BF16), vmem((width, width), BF16),
                vmem(pair, BF16), vmem(pair, BF16), vmem(pair, BF16), vmem(pair, BF16),
                vmem((8, width), F32),
                vmem((2, sub, width), BF16), vmem((2, sub, 3 * width), BF16),
                vmem((2, sub, width), BF16), vmem((2, sub, 3 * cols), BF16),
                vmem((2, sub, width), F32), vmem((2, sub, width), F32),
                vmem((3 * cols, width), F32),
            ],
        ),
        out_shape=(
            jax.ShapeDtypeStruct(x.shape, BF16),
            jax.ShapeDtypeStruct(x.shape, BF16),
            jax.ShapeDtypeStruct((width, 3 * cols), F32),
            jax.ShapeDtypeStruct((cols, width), F32),
            jax.ShapeDtypeStruct((8, width), F32),
        ),
        compiler_params=pltpu.CompilerParams(dimension_semantics=("arbitrary",), vmem_limit_bytes=60 << 20),
        cost_estimate=pl.CostEstimate(
            flops=2 * tokens * width * width * 11, bytes_accessed=8 * tokens * width, transcendentals=0
        ),
        name="main",
    )(me_t, x, g, w, wo, mats, rows, gamma, beta)


def reduce_kernel(
    n_chip, dw_ref, dwo_ref, dgb_ref, dw_out, dwo_out, g_out,
    got_w, got_o, sum_w, sum_o, via_w, via_o, in_w, in_o, gam, in_g,
    a_send, a_recv, g_send, g_recv, b_send, b_recv,
):
    me = lax.axis_index("sp")
    core, chip = lax.rem(me, 2), me // 2
    partner = {"sp": me + 1 - 2 * core}
    right, far, left = (lax.rem(chip + d, n_chip) for d in range(1, n_chip))
    peers = [None] + [{"sp": 2 * c + core} for c in (right, far, left)]
    barrier = pltpu.get_barrier_semaphore()
    for peer in [partner] + peers[1:]:
        pl.semaphore_signal(barrier, inc=1, device_id=peer, device_id_type=MESH)
    for c in range(4):
        gam[0, c : c + 1] = dgb_ref[0:1, c * 128 : (c + 1) * 128]
        gam[0, 4 + c : 5 + c] = dgb_ref[1:2, c * 128 : (c + 1) * 128]
    pl.semaphore_wait(barrier, n_chip)

    def remote(src, dst, send, recv, peer):
        copy = pltpu.make_async_remote_copy(
            src_ref=src, dst_ref=dst, send_sem=send, recv_sem=recv, device_id=peer, device_id_type=MESH
        )
        copy.start()
        return copy

    w_copy = remote(dw_ref.at[:, 1 - core], got_w, a_send.at[0], a_recv.at[0], partner)
    o_copy = remote(dwo_ref.at[:, 1 - core], got_o, a_send.at[1], a_recv.at[1], partner)
    g_copy = remote(gam.at[0], gam.at[1], a_send.at[2], a_recv.at[2], partner)
    w_copy.wait()
    o_copy.wait()
    sum_w[...] = dw_ref[:, core] + got_w[...]
    sum_o[...] = dwo_ref[:, core] + got_o[...]
    hw, ho = sum_w.shape[1] // 2, sum_o.shape[1] // 2
    w_half, o_half = (pl.ds(0, hw), pl.ds(hw, hw)), (pl.ds(0, ho), pl.ds(ho, ho))

    via, near, last = [], [], []
    for h, peer in ((0, peers[1]), (1, peers[3])):
        via.append(remote(sum_w.at[far, w_half[h]], via_w.at[h], b_send.at[0, h], b_recv.at[0, h], peer))
        via.append(remote(sum_o.at[far, o_half[h]], via_o.at[h], b_send.at[1, h], b_recv.at[1, h], peer))
    for h, to, peer in ((0, right, peers[1]), (1, left, peers[3])):
        o = 1 - h
        near.append(remote(sum_w.at[to, w_half[o]], in_w.at[h, w_half[o]], b_send.at[2, h], b_recv.at[2, h], peer))
        near.append(remote(sum_o.at[to, o_half[o]], in_o.at[h, o_half[o]], b_send.at[3, h], b_recv.at[3, h], peer))
    g_copy.wait()
    in_g[0] = gam[0] + gam[1]
    for d in range(1, n_chip):
        near.append(remote(in_g.at[0], in_g.at[d], g_send.at[d], g_recv.at[d], peers[d]))
    for h, to, peer in ((0, right, peers[1]), (1, left, peers[3])):
        via[2 * h].wait()
        via[2 * h + 1].wait()
        sum_w[to, w_half[h]] += via_w[h]
        sum_o[to, o_half[h]] += via_o[h]
        last.append(remote(sum_w.at[to, w_half[h]], in_w.at[h, w_half[h]], b_send.at[4, h], b_recv.at[4, h], peer))
        last.append(remote(sum_o.at[to, o_half[h]], in_o.at[h, o_half[h]], b_send.at[5, h], b_recv.at[5, h], peer))
    for copy in near + last:
        copy.wait()
    w_tot = sum_w[chip] + in_w[0] + in_w[1]
    cols = dw_out.shape[2]
    for e in range(3):
        dw_out[e] = w_tot[:, e * cols : (e + 1) * cols]
    dwo_out[...] = sum_o[chip] + in_o[0] + in_o[1]
    g_tot = in_g[chip]
    for c in range(1, n_chip):
        g_tot = g_tot + in_g[lax.rem(chip - c + n_chip, n_chip)]
    g_out[...] = g_tot


def finish_kernel(dw_ref, dwo_ref, g_ref, gt_ref, dw_out, dwo_out, dg_out, db_out, gt_out):
    dw_out[...] = dw_ref[...]
    dwo_out[...] = dwo_ref[...]
    for c in range(4):
        dg_out[0:1, c * 128 : (c + 1) * 128] = g_ref[c : c + 1]
        db_out[0:1, c * 128 : (c + 1) * 128] = g_ref[4 + c : 5 + c]
    for h in range(gt_ref.shape[0]):
        gt_out[h] = gt_ref[h]


def run_reduce(n_sp, dw, dwo, dgb, grad_temp):
    width, cols3 = dw.shape
    cols = dwo.shape[0]
    n_chip = n_sp // 2
    assert n_chip == 4 and width == 512
    dw = dw.reshape(n_chip, 2, width // n_sp, cols3)
    dwo = dwo.reshape(n_chip, 2, cols // n_sp, width)
    w_shape, o_shape = dw.shape[2:], dwo.shape[2:]
    w_half, o_half = (w_shape[0] // 2, w_shape[1]), (o_shape[0] // 2, o_shape[1])
    spec = pl.BlockSpec(memory_space=pltpu.VMEM)
    smem = pl.BlockSpec(memory_space=pltpu.SMEM)
    vmem, dma = pltpu.VMEM, pltpu.SemaphoreType.DMA
    results = (
        jax.ShapeDtypeStruct((3, width // n_sp, cols3 // 3), F32),
        jax.ShapeDtypeStruct((cols // n_sp, width), F32),
    )
    dw, dwo, g = pl.pallas_call(
        functools.partial(reduce_kernel, n_chip),
        out_shape=results + (jax.ShapeDtypeStruct((8, 128), F32),),
        in_specs=[spec] * 3,
        out_specs=(spec,) * 3,
        scratch_shapes=[
            vmem((n_chip,) + w_shape, F32), vmem((n_chip,) + o_shape, F32),
            vmem((n_chip,) + w_shape, F32), vmem((n_chip,) + o_shape, F32),
            vmem((2,) + w_half, F32), vmem((2,) + o_half, F32),
            vmem((2,) + w_shape, F32), vmem((2,) + o_shape, F32),
            vmem((2, 8, 128), F32), vmem((n_chip, 8, 128), F32),
            dma((3,)), dma((3,)), dma((n_chip,)), dma((n_chip,)), dma((6, 2)), dma((6, 2)),
        ],
        compiler_params=pltpu.CompilerParams(collective_id=1, has_side_effects=True),
        name="reduce",
    )(dw, dwo, dgb)
    row = jax.ShapeDtypeStruct((1, width), F32)
    return pl.pallas_call(
        finish_kernel,
        out_shape=results + (row, row, jax.ShapeDtypeStruct(grad_temp.shape, F32)),
        in_specs=[spec] * 3 + [smem],
        out_specs=(spec,) * 4 + (smem,),
        name="finish",
    )(dw, dwo, g, grad_temp)


def solution(mesh):
    n_tp, n_sp = mesh.shape["tp"], mesh.shape["sp"]
    row_spec = P(("dp", "sp"), None)

    def local_step(x, g, w_qkv, w_out, ln_gamma, ln_beta, temperature):
        width = x.shape[1]
        gamma, beta = ln_gamma.reshape(1, width), ln_beta.reshape(1, width)
        me_t = lax.axis_index("tp").astype(jnp.int32).reshape(1)
        w, wo, mats, rows, grad_temp = run_state(
            n_sp, n_tp, x, g, w_qkv.transpose(1, 0, 2), w_out, gamma, beta, temperature
        )
        y, dx, dw, dwo, dgb = run_main(n_tp, me_t, x, g, w, wo, mats, rows, gamma, beta)
        dw, dwo, dgamma, dbeta, grad_temp = run_reduce(n_sp, dw, dwo, dgb, grad_temp)
        return y, dx, dw.transpose(1, 0, 2), dwo, dgamma.reshape(-1), dbeta.reshape(-1), grad_temp

    in_specs = (row_spec, row_spec, P(None, None, "tp"), P("tp", None), P(None), P(None), P(None))
    out_specs = (row_spec, row_spec, P(("dp", "sp"), None, "tp"), P(("dp", "tp", "sp"), None), P("dp"), P("dp"), P("dp"))
    return jax.shard_map(local_step, mesh=mesh, in_specs=in_specs, out_specs=out_specs, check_vma=False)
```

```python
import functools

import jax
import jax.numpy as jnp
from jax import lax
from jax.experimental import pallas as pl
from jax.experimental.pallas import tpu as pltpu
from jax.sharding import PartitionSpec as P

LN_EPS = 1e-6
F32 = jnp.float32
BF16 = jnp.bfloat16
MESH = pl.DeviceIdType.MESH
STATS_ROWS = 4096
STATS_SUB = 1024
CHUNK = 128
MAIN_ROWS = 2048
MAIN_SUB = 512


def dot(lhs, rhs):
    return jnp.dot(lhs, rhs, preferred_element_type=F32)


def dot_rows(lhs, rhs):
    return lax.dot_general(lhs, rhs, (((0,), (0,)), ((), ())), preferred_element_type=F32)


def dot_cols(lhs, rhs):
    return lax.dot_general(lhs, rhs, (((1,), (1,)), ((), ())), preferred_element_type=F32)


def layer_norm(x, gamma, beta):
    centered = x - jnp.mean(x, axis=-1, keepdims=True)
    inv_std = lax.rsqrt(jnp.mean(centered * centered, axis=-1, keepdims=True) + LN_EPS)
    x_hat = centered * inv_std
    return x_hat, inv_std, (x_hat * gamma + beta).astype(BF16)


def weave(steps, *sides):
    order = [((i + 0.5) / len(steps), 0, i, f) for i, f in enumerate(steps)]
    for n, side in enumerate(sides):
        order += [((i + 0.25) / len(side), n + 1, i, f) for i, f in enumerate(side)]
    for *_, f in sorted(order, key=lambda e: e[:3]):
        f()


def state_kernel(
    n_sp, n_tp, x_ref, g_ref, w_ref, wo_ref, gamma_ref, beta_ref, temp_ref, w_any, wo_any,
    w_all, wo_all, mats_ref, rows_ref, gt_ref,
    wt_s, wot_s, u_s, qk_s, vd_s, pair, got, gath, mats, rows,
    w_send, w_recv, p_send, p_recv, w_local, pair_send, pair_recv, sp_send, sp_recv, tp_send, tp_recv,
):
    step = pl.program_id(0)
    me_s, me_t = lax.axis_index("sp"), lax.axis_index("tp")
    n_chip = n_sp // 2
    core, chip = lax.rem(me_s, 2), me_s // 2
    cols, width = wo_ref.shape
    hd = cols // 2
    partner = {"sp": me_s + 1 - 2 * core}
    chips = [{"sp": 2 * lax.rem(chip + d, n_chip) + core} for d in range(n_chip)]
    tps = [{"tp": lax.rem(me_t + d, n_tp)} for d in range(n_tp)]

    n_rows, n_wo = w_any.shape[1] // 2, wo_any.shape[0] // 2
    rows_of = pl.ds(pl.multiple_of(core * n_rows, n_rows), n_rows)
    wo_of = pl.ds(pl.multiple_of(core * n_wo, n_wo), n_wo)

    def gather_copies():
        copies = []
        for d in range(1, n_tp):
            for k, (src, dst) in enumerate(
                ((w_any.at[:, rows_of], w_all.at[me_t, :, rows_of]), (wo_any.at[wo_of], wo_all.at[me_t, wo_of]))
            ):
                copies.append(pltpu.make_async_remote_copy(
                    src_ref=src, dst_ref=dst, send_sem=w_send.at[k, d], recv_sem=w_recv.at[k, d],
                    device_id=tps[d], device_id_type=MESH,
                ))
        return copies

    def pass_copies():
        copies = []
        for d in range(1, n_tp):
            t = lax.rem(me_t - d + n_tp, n_tp)
            for k, ref in enumerate((w_all.at[t, :, rows_of], wo_all.at[t, wo_of])):
                copies.append(pltpu.make_async_remote_copy(
                    src_ref=ref, dst_ref=ref, send_sem=p_send.at[k, d], recv_sem=p_recv.at[k, d],
                    device_id=partner, device_id_type=MESH,
                ))
        return copies

    def local_copies():
        return [
            pltpu.make_async_copy(src, dst.at[me_t], w_local.at[k])
            for k, (src, dst) in enumerate(((w_any, w_all), (wo_any, wo_all)))
        ]

    @pl.when(step == 0)
    def _():
        barrier = pltpu.get_barrier_semaphore()
        others = [{"tp": peer["tp"], "sp": partner["sp"]} for peer in tps[1:]]
        for peer in [partner] + chips[1:] + tps[1:] + others:
            pl.semaphore_signal(barrier, inc=1, device_id=peer, device_id_type=MESH)
        pl.semaphore_wait(barrier, n_chip + 2 * n_tp - 2)
        for copy in gather_copies() + local_copies():
            copy.start()
        for e in range(3):
            wt_s[e * cols : (e + 1) * cols, :] = w_ref[e].T
        wot_s[...] = wo_ref[...].T
        qk_s[...] = jnp.zeros_like(qk_s)
        vd_s[...] = jnp.zeros_like(vd_s)

    @pl.when(step == pl.num_programs(0) - 1)
    def _():
        for copy in gather_copies():
            copy.wait()
        for copy in pass_copies():
            copy.start()

    sub = u_s.shape[1]
    n_sub = x_ref.shape[0] // sub
    gamma, beta = gamma_ref[...], beta_ref[...]

    def norm(s):
        def piece(at):
            x = x_ref[s * sub + at : s * sub + at + CHUNK].astype(F32)
            u_s[s % 2, at : at + CHUNK] = layer_norm(x, gamma, beta)[2]

        return [functools.partial(piece, at) for at in range(0, sub, CHUNK)]

    def sums(s):
        qkv = dot_cols(wt_s[...], u_s[s % 2]).astype(BF16)
        qk_s[...] += dot_cols(qkv[: 2 * cols], qkv[: 2 * cols])
        dout = dot(g_ref[s * sub : (s + 1) * sub], wot_s[...]).astype(BF16)
        vd_s[...] += dot(qkv[2 * cols :], dout)

    weave(norm(0))
    for s in range(n_sub):
        if s + 1 < n_sub:
            weave(norm(s + 1))
        sums(s)

    @pl.when(step == pl.num_programs(0) - 1)
    def _():
        first = lax.broadcasted_iota(jnp.int32, (hd, cols), 1) < hd
        eye = lax.broadcasted_iota(jnp.int32, (cols, cols), 0) == lax.broadcasted_iota(jnp.int32, (cols, cols), 1)

        def diag_row(block):
            return jnp.sum(jnp.where(eye, block, 0.0), axis=0, keepdims=True)

        gram, d_attn = qk_s[:cols, cols:], vd_s[...].T
        q_row, k_row = diag_row(qk_s[:cols, :cols]), diag_row(qk_s[cols:, cols:])
        for h in range(2):
            g_h, d_h = gram[h * hd : (h + 1) * hd], d_attn[h * hd : (h + 1) * hd]
            if h == 0:
                top, low = jnp.where(first, g_h, pltpu.roll(d_h, hd, 1)), (q_row, pltpu.roll(jnp.broadcast_to(k_row, (8, cols)), hd, 1)[:1])
            else:
                top, low = jnp.where(first, pltpu.roll(g_h, hd, 1), d_h), (pltpu.roll(jnp.broadcast_to(q_row, (8, cols)), hd, 1)[:1], k_row)
            pair[h, :hd] = top
            pair[h, hd:] = jnp.broadcast_to(jnp.where(first[:1], low[0], low[1]), (8, cols))
        copy = pltpu.make_async_remote_copy(
            src_ref=pair.at[1 - core], dst_ref=got, send_sem=pair_send, recv_sem=pair_recv,
            device_id=partner, device_id_type=MESH,
        )
        copy.start()
        copy.wait()
        gath[0] = pair[core] + got[...]
        copies = []
        for d in range(1, n_chip):
            copy = pltpu.make_async_remote_copy(
                src_ref=gath.at[0], dst_ref=gath.at[d], send_sem=sp_send.at[d], recv_sem=sp_recv.at[d],
                device_id=chips[d], device_id_type=MESH,
            )
            copy.start()
            copies.append(copy)
        for copy in copies:
            copy.wait()
        total = gath[chip]
        for c in range(1, n_chip):
            total = total + gath[lax.rem(chip - c + n_chip, n_chip)]

        gram, d_attn = total[:hd, :hd], total[:hd, hd:]
        q_row, k_row = total[hd : hd + 1, :hd], total[hd : hd + 1, hd:]
        same = lax.broadcasted_iota(jnp.int32, (hd, hd), 0) == lax.broadcasted_iota(jnp.int32, (hd, hd), 1)

        def to_col(row):
            return jnp.sum(jnp.where(same, jnp.broadcast_to(row, (hd, hd)), 0.0), axis=1, keepdims=True)

        def to_row(col):
            return jnp.sum(jnp.where(same, jnp.broadcast_to(col, (hd, hd)), 0.0), axis=0, keepdims=True)

        q_col = to_col(q_row)
        temp = temp_ref[2 * me_t + core]
        norm_prod = jnp.sqrt(q_col) * jnp.sqrt(k_row)
        gram_n = gram / norm_prod
        logit = temp * gram_n
        expo = jnp.exp(logit - jnp.max(logit, axis=1, keepdims=True))
        attn = expo / jnp.sum(expo, axis=1, keepdims=True)
        d_logit = attn * (d_attn - jnp.sum(attn * d_attn, axis=1, keepdims=True))
        temp_part = jnp.sum(jnp.sum(d_logit * gram_n, axis=1, keepdims=True), axis=0, keepdims=True)
        grad_sn = temp * d_logit
        prod = grad_sn * gram_n
        q_coef = to_row(-jnp.sum(prod, axis=1, keepdims=True) / q_col)
        k_coef = -jnp.sum(prod, axis=0, keepdims=True) / k_row

        mats[0] = jnp.concatenate([attn, grad_sn / norm_prod], axis=1).astype(BF16)
        rows[0] = jnp.concatenate(
            [jnp.concatenate([q_coef, k_coef], axis=1), jnp.broadcast_to(temp_part, (7, cols))], axis=0
        )
        copies = []
        for d in range(n_tp):
            for j in range(2):
                if d + j > 0:
                    slot = 2 * d + j
                    to = {"tp": lax.rem(me_t + d, n_tp), "sp": me_s + j * (1 - 2 * core)}
                    for k, ref in enumerate((mats, rows)):
                        copy = pltpu.make_async_remote_copy(
                            src_ref=ref.at[0], dst_ref=ref.at[slot], send_sem=tp_send.at[k, slot],
                            recv_sem=tp_recv.at[k, slot], device_id=to, device_id_type=MESH,
                        )
                        copy.start()
                        copies.append(copy)
        for copy in copies:
            copy.wait()
        for t in range(n_tp):
            for c in range(2):
                slot = 2 * lax.rem(me_t - t + n_tp, n_tp) + core + c - 2 * core * c
                mats_ref[2 * t + c] = mats[slot]
                part = rows[slot]
                rows_ref[2 * t + c] = part
                gt_ref[2 * t + c] = part[1, 0]
        for copy in pass_copies() + local_copies():
            copy.wait()


def run_state(n_sp, n_tp, x, g, w, wo, gamma, beta, temp):
    tokens, width = x.shape
    cols = wo.shape[0]
    hd = cols // 2
    r, sub = STATS_ROWS, STATS_SUB
    tile = pl.BlockSpec((r, width), lambda i: (i, 0))

    def whole(shape):
        return pl.BlockSpec(shape, lambda i: (0,) * len(shape))

    hbm = pl.BlockSpec(memory_space=pl.ANY)
    smem = pl.BlockSpec(memory_space=pltpu.SMEM)
    vmem, dma = pltpu.VMEM, pltpu.SemaphoreType.DMA
    return pl.pallas_call(
        functools.partial(state_kernel, n_sp, n_tp),
        grid=(tokens // r,),
        out_shape=(
            jax.ShapeDtypeStruct((n_tp,) + w.shape, BF16),
            jax.ShapeDtypeStruct((n_tp,) + wo.shape, BF16),
            jax.ShapeDtypeStruct((2 * n_tp, hd, cols), BF16),
            jax.ShapeDtypeStruct((2 * n_tp, 8, cols), F32),
            jax.ShapeDtypeStruct(temp.shape, F32),
        ),
        in_specs=[tile, tile, whole(w.shape), whole(wo.shape), whole((1, width)), whole((1, width)), smem, hbm, hbm],
        out_specs=(hbm, hbm, whole((2 * n_tp, hd, cols)), whole((2 * n_tp, 8, cols)), smem),
        scratch_shapes=[
            vmem((3 * cols, width), BF16), vmem((width, cols), BF16), vmem((2, sub, width), BF16),
            vmem((2 * cols, 2 * cols), F32), vmem((cols, cols), F32),
            vmem((2, hd + 8, cols), F32), vmem((hd + 8, cols), F32), vmem((n_sp // 2, hd + 8, cols), F32),
            vmem((2 * n_tp, hd, cols), BF16), vmem((2 * n_tp, 8, cols), F32),
            dma((2, n_tp)), dma((2, n_tp)), dma((2, n_tp)), dma((2, n_tp)), dma((2,)), dma, dma, dma((n_sp // 2,)), dma((n_sp // 2,)),
            dma((2, 2 * n_tp)), dma((2, 2 * n_tp)),
        ],
        compiler_params=pltpu.CompilerParams(
            dimension_semantics=("arbitrary",), vmem_limit_bytes=60 << 20, collective_id=0, has_side_effects=True
        ),
        name="state",
    )(x, g, w, wo, gamma, beta, temp, w, wo)


def main_kernel(
    n_tp, t_ref, x_ref, g_ref, w_ref, wo_ref, mats_ref, rows_ref, gamma_ref, beta_ref,
    y_ref, dx_ref, dw_ref, dwo_ref, dgb_ref,
    w_s, wt_s, wo_s, wot_s, at_s, a_s, gt_s, g_s, co_s, u_s, r_s, o_s, own_s, xh_s, du_s, dwt_s,
):
    width = x_ref.shape[1]
    cols = width // n_tp
    hd = cols // 2
    me_t = t_ref[0]
    step = pl.program_id(0)

    @pl.when(step == 0)
    def _():
        for t in range(n_tp):
            at = t * cols
            for e in range(3):
                w_s[:, e * width + at : e * width + at + cols] = w_ref[t, e]
                wt_s[e * width + at : e * width + at + cols, :] = w_ref[t, e].T
            wo_s[at : at + cols, :] = wo_ref[t]
            wot_s[:, at : at + cols] = wo_ref[t].T
        for ref in (at_s, a_s, gt_s, g_s):
            ref[...] = jnp.zeros_like(ref)
        first = lax.broadcasted_iota(jnp.int32, (hd, cols), 1) < hd
        for t in range(n_tp):
            p, off = t // 2, (t % 2) * cols
            even, odd = mats_ref[2 * t].astype(F32), mats_ref[2 * t + 1].astype(F32)
            for plain, trans, hi, lo in (
                (a_s, at_s, even, pltpu.roll(odd, hd, 1)), (g_s, gt_s, pltpu.roll(even, hd, 1), odd)
            ):
                full = jnp.concatenate([jnp.where(first, hi, 0.0), jnp.where(first, 0.0, lo)], axis=0)
                plain[p, off : off + cols, off : off + cols] = full.astype(BF16)
                trans[p, off : off + cols, off : off + cols] = full.T.astype(BF16)
            pair = [rows_ref[2 * t, 0:1], rows_ref[2 * t + 1, 0:1]]
            turned = [pltpu.roll(jnp.broadcast_to(row, (8, cols)), hd, 1)[:1] for row in pair]
            at = slice(t * cols, (t + 1) * cols)
            co_s[0:1, at] = jnp.where(first[:1], pair[0], turned[1])
            co_s[1:2, at] = jnp.where(first[:1], turned[0], pair[1])
        dwt_s[...] = jnp.zeros_like(dwt_s)
        dwo_ref[...] = jnp.zeros_like(dwo_ref)
        dgb_ref[...] = jnp.zeros_like(dgb_ref)

    sub = u_s.shape[1]
    n_sub = x_ref.shape[0] // sub
    gamma, beta = gamma_ref[...], beta_ref[...]
    mine = pl.multiple_of(me_t * cols, cols)

    def norm(s):
        x_hat, inv_std, u = layer_norm(x_ref[s * sub : (s + 1) * sub].astype(F32), gamma, beta)
        xh_s[s % 2] = x_hat
        u_s[s % 2] = u
        return inv_std

    def attend(s):
        b, at = s % 2, slice(s * sub, (s + 1) * sub)
        for p in range(2):
            lo, hi = p * 2 * cols, (p + 1) * 2 * cols
            q = dot(u_s[b], w_s[:, lo:hi]).astype(BF16)
            k = dot(u_s[b], w_s[:, width + lo : width + hi]).astype(BF16)
            v = dot(u_s[b], w_s[:, 2 * width + lo : 2 * width + hi]).astype(BF16)
            dout = dot(g_ref[at], wot_s[:, lo:hi]).astype(BF16)
            o_s[b, :, lo:hi] = dot(v, at_s[p]).astype(BF16)
            r_s[b, :, 2 * width + lo : 2 * width + hi] = dot(dout, a_s[p]).astype(BF16)
            r_s[b, :, lo:hi] = (dot(k, gt_s[p]) + q.astype(F32) * co_s[0:1, lo:hi]).astype(BF16)
            r_s[b, :, width + lo : width + hi] = (dot(q, g_s[p]) + k.astype(F32) * co_s[1:2, lo:hi]).astype(BF16)
        y_ref[at] = (x_ref[at].astype(F32) + dot(o_s[b], wo_s[...])).astype(BF16)
        du_s[b] = dot(r_s[b], wt_s[...])

    def weights(s):
        b, at = s % 2, slice(s * sub, (s + 1) * sub)
        for e in range(3):
            own_s[b, :, e * cols : (e + 1) * cols] = r_s[b, :, pl.ds(e * width + mine, cols)]
        dwt_s[...] += dot_rows(own_s[b], u_s[b])
        dwo_ref[...] += dot_rows(o_s[b, :, pl.ds(mine, cols)], g_ref[at])

    def norm_grad(s, inv_std):
        b, at = s % 2, slice(s * sub, (s + 1) * sub)
        du, x_hat = du_s[b], xh_s[b]
        dgb_ref[0:1] += jnp.sum(du * x_hat, axis=0, keepdims=True)
        dgb_ref[1:2] += jnp.sum(du, axis=0, keepdims=True)
        gx = du * gamma
        mean1 = jnp.mean(gx, axis=-1, keepdims=True)
        mean2 = jnp.mean(gx * x_hat, axis=-1, keepdims=True)
        dx_ref[at] = (g_ref[at].astype(F32) + inv_std * (gx - mean1 - x_hat * mean2)).astype(BF16)

    inv = {0: norm(0)}
    for s in range(n_sub):
        if s + 1 < n_sub:
            inv[s + 1] = norm(s + 1)
        attend(s)
        norm_grad(s, inv[s])
        weights(s)

    @pl.when(step == pl.num_programs(0) - 1)
    def _():
        for e in range(3):
            dw_ref[:, e * cols : (e + 1) * cols] = dwt_s[e * cols : (e + 1) * cols, :].T


def run_main(n_tp, me_t, x, g, w, wo, mats, rows, gamma, beta):
    tokens, width = x.shape
    cols = width // n_tp
    r, sub = MAIN_ROWS, MAIN_SUB
    tile = pl.BlockSpec((r, width), lambda i, t: (i, 0))

    def whole(shape):
        return pl.BlockSpec(shape, lambda i, t: (0,) * len(shape))

    vmem = pltpu.VMEM
    pair = (2, 2 * cols, 2 * cols)
    return pl.pallas_call(
        functools.partial(main_kernel, n_tp),
        grid_spec=pltpu.PrefetchScalarGridSpec(
            num_scalar_prefetch=1,
            grid=(tokens // r,),
            in_specs=[tile, tile] + [whole(a.shape) for a in (w, wo, mats, rows, gamma, beta)],
            out_specs=(tile, tile, whole((width, 3 * cols)), whole((cols, width)), whole((8, width))),
            scratch_shapes=[
                vmem((width, 3 * width), BF16), vmem((3 * width, width), BF16),
                vmem((width, width), BF16), vmem((width, width), BF16),
                vmem(pair, BF16), vmem(pair, BF16), vmem(pair, BF16), vmem(pair, BF16),
                vmem((8, width), F32),
                vmem((2, sub, width), BF16), vmem((2, sub, 3 * width), BF16),
                vmem((2, sub, width), BF16), vmem((2, sub, 3 * cols), BF16),
                vmem((2, sub, width), F32), vmem((2, sub, width), F32),
                vmem((3 * cols, width), F32),
            ],
        ),
        out_shape=(
            jax.ShapeDtypeStruct(x.shape, BF16),
            jax.ShapeDtypeStruct(x.shape, BF16),
            jax.ShapeDtypeStruct((width, 3 * cols), F32),
            jax.ShapeDtypeStruct((cols, width), F32),
            jax.ShapeDtypeStruct((8, width), F32),
        ),
        compiler_params=pltpu.CompilerParams(dimension_semantics=("arbitrary",), vmem_limit_bytes=60 << 20),
        cost_estimate=pl.CostEstimate(
            flops=2 * tokens * width * width * 11, bytes_accessed=8 * tokens * width, transcendentals=0
        ),
        name="main",
    )(me_t, x, g, w, wo, mats, rows, gamma, beta)


def reduce_kernel(
    n_chip, dw_any, dwo_any, dgb_ref, dw_out, dwo_out, g_out,
    dw_ref, dwo_ref, got_w, got_o, sum_w, sum_o, via_w, via_o, in_w, in_o, gam, in_g,
    l_sem, a_send, a_recv, g_send, g_recv, b_send, b_recv,
):
    me = lax.axis_index("sp")
    core, chip = lax.rem(me, 2), me // 2
    partner = {"sp": me + 1 - 2 * core}
    right, far, left = (lax.rem(chip + d, n_chip) for d in range(1, n_chip))
    peers = [None] + [{"sp": 2 * c + core} for c in (right, far, left)]
    barrier = pltpu.get_barrier_semaphore()
    for peer in [partner] + peers[1:]:
        pl.semaphore_signal(barrier, inc=1, device_id=peer, device_id_type=MESH)
    loads = [
        pltpu.make_async_copy(src, dst, l_sem.at[k])
        for k, (src, dst) in enumerate(((dw_any, dw_ref), (dwo_any, dwo_ref)))
    ]
    for copy in loads:
        copy.start()
    for c in range(4):
        gam[0, c : c + 1] = dgb_ref[0:1, c * 128 : (c + 1) * 128]
        gam[0, 4 + c : 5 + c] = dgb_ref[1:2, c * 128 : (c + 1) * 128]
    for copy in loads:
        copy.wait()
    pl.semaphore_wait(barrier, n_chip)

    def remote(src, dst, send, recv, peer):
        copy = pltpu.make_async_remote_copy(
            src_ref=src, dst_ref=dst, send_sem=send, recv_sem=recv, device_id=peer, device_id_type=MESH
        )
        copy.start()
        return copy

    order = (far, right, left, chip)
    halves = []
    for i, c in enumerate(order):
        halves.append((
            remote(dw_ref.at[c, 1 - core], got_w.at[c], a_send.at[0, i], a_recv.at[0, i], partner),
            remote(dwo_ref.at[c, 1 - core], got_o.at[c], a_send.at[1, i], a_recv.at[1, i], partner),
        ))
    g_copy = remote(gam.at[0], gam.at[1], a_send.at[2, 0], a_recv.at[2, 0], partner)

    def join(i):
        c = order[i]
        for copy in halves[i]:
            copy.wait()
        sum_w[c] = dw_ref[c, core] + got_w[c]
        sum_o[c] = dwo_ref[c, core] + got_o[c]

    join(0)
    hw, ho = sum_w.shape[1] // 2, sum_o.shape[1] // 2
    w_half, o_half = (pl.ds(0, hw), pl.ds(hw, hw)), (pl.ds(0, ho), pl.ds(ho, ho))

    via, near, last = [], [], []
    for h, peer in ((0, peers[1]), (1, peers[3])):
        via.append(remote(sum_w.at[far, w_half[h]], via_w.at[h], b_send.at[0, h], b_recv.at[0, h], peer))
        via.append(remote(sum_o.at[far, o_half[h]], via_o.at[h], b_send.at[1, h], b_recv.at[1, h], peer))
    join(1)
    join(2)
    for h, to, peer in ((0, right, peers[1]), (1, left, peers[3])):
        o = 1 - h
        near.append(remote(sum_w.at[to, w_half[o]], in_w.at[h, w_half[o]], b_send.at[2, h], b_recv.at[2, h], peer))
        near.append(remote(sum_o.at[to, o_half[o]], in_o.at[h, o_half[o]], b_send.at[3, h], b_recv.at[3, h], peer))
    join(3)
    g_copy.wait()
    in_g[0] = gam[0] + gam[1]
    for d in range(1, n_chip):
        near.append(remote(in_g.at[0], in_g.at[d], g_send.at[d], g_recv.at[d], peers[d]))
    for h, to, peer in ((0, right, peers[1]), (1, left, peers[3])):
        via[2 * h].wait()
        via[2 * h + 1].wait()
        sum_w[to, w_half[h]] += via_w[h]
        sum_o[to, o_half[h]] += via_o[h]
        last.append(remote(sum_w.at[to, w_half[h]], in_w.at[h, w_half[h]], b_send.at[4, h], b_recv.at[4, h], peer))
        last.append(remote(sum_o.at[to, o_half[h]], in_o.at[h, o_half[h]], b_send.at[5, h], b_recv.at[5, h], peer))
    for copy in near + last:
        copy.wait()
    w_tot = sum_w[chip] + in_w[0] + in_w[1]
    cols = dw_out.shape[2]
    for e in range(3):
        dw_out[e] = w_tot[:, e * cols : (e + 1) * cols]
    dwo_out[...] = sum_o[chip] + in_o[0] + in_o[1]
    g_tot = in_g[chip]
    for c in range(1, n_chip):
        g_tot = g_tot + in_g[lax.rem(chip - c + n_chip, n_chip)]
    g_out[...] = g_tot


def finish_kernel(dw_ref, dwo_ref, g_ref, gt_ref, dw_out, dwo_out, dg_out, db_out, gt_out):
    dw_out[...] = dw_ref[...]
    dwo_out[...] = dwo_ref[...]
    for c in range(4):
        dg_out[0:1, c * 128 : (c + 1) * 128] = g_ref[c : c + 1]
        db_out[0:1, c * 128 : (c + 1) * 128] = g_ref[4 + c : 5 + c]
    for h in range(gt_ref.shape[0]):
        gt_out[h] = gt_ref[h]


def run_reduce(n_sp, dw, dwo, dgb, grad_temp):
    width, cols3 = dw.shape
    cols = dwo.shape[0]
    n_chip = n_sp // 2
    assert n_chip == 4 and width == 512
    dw = dw.reshape(n_chip, 2, width // n_sp, cols3)
    dwo = dwo.reshape(n_chip, 2, cols // n_sp, width)
    w_shape, o_shape = dw.shape[2:], dwo.shape[2:]
    w_half, o_half = (w_shape[0] // 2, w_shape[1]), (o_shape[0] // 2, o_shape[1])
    spec = pl.BlockSpec(memory_space=pltpu.VMEM)
    smem = pl.BlockSpec(memory_space=pltpu.SMEM)
    vmem, dma = pltpu.VMEM, pltpu.SemaphoreType.DMA
    results = (
        jax.ShapeDtypeStruct((3, width // n_sp, cols3 // 3), F32),
        jax.ShapeDtypeStruct((cols // n_sp, width), F32),
    )
    dw, dwo, g = pl.pallas_call(
        functools.partial(reduce_kernel, n_chip),
        out_shape=results + (jax.ShapeDtypeStruct((8, 128), F32),),
        in_specs=[pl.BlockSpec(memory_space=pl.ANY)] * 2 + [spec],
        out_specs=(spec,) * 3,
        scratch_shapes=[
            vmem(dw.shape, F32), vmem(dwo.shape, F32),
            vmem((n_chip,) + w_shape, F32), vmem((n_chip,) + o_shape, F32),
            vmem((n_chip,) + w_shape, F32), vmem((n_chip,) + o_shape, F32),
            vmem((2,) + w_half, F32), vmem((2,) + o_half, F32),
            vmem((2,) + w_shape, F32), vmem((2,) + o_shape, F32),
            vmem((2, 8, 128), F32), vmem((n_chip, 8, 128), F32),
            dma((2,)), dma((3, n_chip)), dma((3, n_chip)), dma((n_chip,)), dma((n_chip,)), dma((6, 2)), dma((6, 2)),
        ],
        compiler_params=pltpu.CompilerParams(collective_id=1, has_side_effects=True),
        name="reduce",
    )(dw, dwo, dgb)
    row = jax.ShapeDtypeStruct((1, width), F32)
    return pl.pallas_call(
        finish_kernel,
        out_shape=results + (row, row, jax.ShapeDtypeStruct(grad_temp.shape, F32)),
        in_specs=[spec] * 3 + [smem],
        out_specs=(spec,) * 4 + (smem,),
        name="finish",
    )(dw, dwo, g, grad_temp)


def solution(mesh):
    n_tp, n_sp = mesh.shape["tp"], mesh.shape["sp"]
    row_spec = P(("dp", "sp"), None)

    def local_step(x, g, w_qkv, w_out, ln_gamma, ln_beta, temperature):
        width = x.shape[1]
        gamma, beta = ln_gamma.reshape(1, width), ln_beta.reshape(1, width)
        me_t = lax.axis_index("tp").astype(jnp.int32).reshape(1)
        w, wo, mats, rows, grad_temp = run_state(
            n_sp, n_tp, x, g, w_qkv.transpose(1, 0, 2), w_out, gamma, beta, temperature
        )
        y, dx, dw, dwo, dgb = run_main(n_tp, me_t, x, g, w, wo, mats, rows, gamma, beta)
        dw, dwo, dgamma, dbeta, grad_temp = run_reduce(n_sp, dw, dwo, dgb, grad_temp)
        return y, dx, dw.transpose(1, 0, 2), dwo, dgamma.reshape(-1), dbeta.reshape(-1), grad_temp

    in_specs = (row_spec, row_spec, P(None, None, "tp"), P("tp", None), P(None), P(None), P(None))
    out_specs = (row_spec, row_spec, P(("dp", "sp"), None, "tp"), P(("dp", "tp", "sp"), None), P("dp"), P("dp"), P("dp"))
    return jax.shard_map(local_step, mesh=mesh, in_specs=in_specs, out_specs=out_specs, check_vma=False)
```
